32 devices in a mesh: group: 8 (over z, x), peer: 4 (over y, core).
Axes of the slice: x: 2, y: 2, z: 4, core: 2. Of those that a mesh axis runs over, the one named last changes fastest.
Arguments:
- features: bfloat16 [12288, 1024], P(('group', 'peer')), may hold values from -6 to 6
- task_mask: int32 [12288], P(('group', 'peer')), may hold values from 0 to 65535, as said below
- tower_in: bfloat16 [16, 2048, 1024], P('peer', 'group'), may hold values from -0.1875 to 0.1875
- tower_bias: bfloat16 [16, 2048], P('peer', 'group'), may hold values from -5 to 5
- tower_head: bfloat16 [16, 2048], P('peer', 'group'), may hold values from -0.125 to 0.125
- head_bias: float32 [16], P('peer'), may hold values from -4 to 4
Outputs:
- predictions: float32 [12288, 16], P(('group', 'peer'))
The draws below stay inside these ranges and needn't reach their ends.
Inputs may be any that keep to these rules, and one draw needn't show every extreme that they name: `task_mask`: only bits 0 to 15 are used. Among the 384 samples of one device (aligned blocks of 384), at most 176 have any one bit set; in every run of 4 blocks that one group holds, some task's bit is set exactly 176 times in each block.
All inputs are finite; a program needn't handle non-finite values.
Results may differ from the reference program's by a relative error of at most 0.0003.
Values may be sent and summed in bfloat16 or wider, within the bound.
A program may use at most 128 MiB of HBM per device.

```python
import jax
import jax.numpy as jnp
from jax import lax

D = 1024
H = 2048
CAP = 176
SAMP_DEV = 384
TASKS = 16
SAMPLES = 12288
N_PEER = 4


def draw_task_mask(key, part):
    blocks = SAMPLES // SAMP_DEV
    groups = blocks // N_PEER
    hot_task = jax.random.randint(jax.random.fold_in(key, 11), (groups,), 0, TASKS)
    active_block = jnp.repeat(hot_task, N_PEER)
    spread = jax.random.randint(jax.random.fold_in(key, 12), (blocks, TASKS), 0, CAP + 1)
    counts = spread * spread // CAP
    task_ids = jnp.arange(TASKS, dtype=jnp.int32)
    counts = jnp.where(task_ids[None, :] == active_block[:, None], CAP, counts)
    keys = jax.random.split(jax.random.fold_in(key, 13), blocks * TASKS)
    sort_orders = jax.vmap(lambda single: jax.random.permutation(single, SAMP_DEV))(keys)
    sort_orders = sort_orders.reshape(blocks, TASKS, SAMP_DEV).astype(jnp.int32)
    task_bits = (sort_orders < counts[:, :, None]).astype(jnp.int32)
    packed = jnp.sum(task_bits << task_ids[None, :, None], axis=1)
    return packed.reshape(-1).astype(jnp.int32)


def levels(own_key, dims, cuts, low, top_value):
    def one(dim, blocks):
        steps = jax.random.uniform(jax.random.fold_in(jax.random.fold_in(own_key, 6), dim), (blocks,), jnp.float32, low / len(cuts), top_value / len(cuts))
        return jnp.repeat(jnp.exp(steps), dims[dim] // blocks).reshape((-1,) + (1,) * (len(dims) - dim - 1))

    level = one(*cuts[0])
    for cut in cuts[1:]:
        level = level * one(*cut)
    return level


def scatter_about(stream_key, extent, scale, limit, pieces=(), held_as=jnp.bfloat16):
    gain = levels(stream_key, extent, pieces, -0.22, 0.18) if pieces else 1.0
    values = jax.random.normal(stream_key, extent, jnp.float32) * scale * gain
    return jnp.minimum(jnp.maximum(values, -limit), limit).astype(held_as)


def setup_inputs(seed: int = 0) -> dict:
    key_list = jax.random.split(jax.random.key(seed), 7)
    features = scatter_about(key_list[0], (SAMPLES, D), 1.0, 6.0, ((0, 32),))
    task_mask = draw_task_mask(jax.random.fold_in(key_list[6], 71), 0)
    tower_in = scatter_about(key_list[2], (TASKS, H, D), D ** -0.5, 0.1875, ((0, 4), (1, 8)))
    tower_bias = scatter_about(key_list[3], (TASKS, H), 1.0, 5.0, ((0, 4), (1, 8)))
    tower_head = scatter_about(key_list[4], (TASKS, H), H ** -0.5, 0.125, ((0, 4), (1, 8)))
    head_bias = scatter_about(key_list[5], (TASKS,), 1.0, 4.0, ((0, 4),), jnp.float32)
    return dict(features=features, task_mask=task_mask, tower_in=tower_in, tower_bias=tower_bias, tower_head=tower_head, head_bias=head_bias)


def block_logits(block_rows, block_mask, layer_entry, hidden_unit_bias, head_rows, out_bias):
    sample_count = block_rows.shape[0]
    task_ids = jnp.arange(TASKS, dtype=jnp.int32)
    task_bits = (block_mask[:, None] >> task_ids[None, :]) & 1
    inclusive = jnp.cumsum(task_bits, axis=0)
    slot_rank = inclusive - task_bits
    slot_indices = jnp.arange(CAP, dtype=jnp.int32)
    sample_index = jnp.sum((inclusive[:, :, None] <= slot_indices[None, None, :]).astype(jnp.int32), axis=0)
    sample_index = jnp.clip(sample_index, 0, sample_count - 1).astype(jnp.int32)
    gathered = block_rows.astype(jnp.float32)[sample_index]
    preact = jnp.einsum("tcd,thd->tch", gathered, layer_entry, precision=lax.Precision.HIGHEST)
    hidden = jnp.maximum(preact + hidden_unit_bias[:, None, :], 0.0)
    logit = jnp.sum(hidden * head_rows[:, None, :], axis=-1) + out_bias[:, None]
    picked = logit[task_ids[None, :], jnp.clip(slot_rank, 0, CAP - 1).astype(jnp.int32)]
    return jnp.where(task_bits == 1, picked, jnp.float32(0.0))


def reference(features, task_mask, tower_in, tower_bias, tower_head, head_bias):
    blocks = SAMPLES // SAMP_DEV
    layer_entry = tower_in.astype(jnp.float32)
    hidden_unit_bias = tower_bias.astype(jnp.float32)
    head_rows = tower_head.astype(jnp.float32)
    rows_blocked = features.reshape(blocks, SAMP_DEV, D)
    mask_blocked = task_mask.reshape(blocks, SAMP_DEV)

    def one_block(pair):
        return block_logits(pair[0], pair[1], layer_entry, hidden_unit_bias, head_rows, head_bias)

    result = lax.map(one_block, (rows_blocked, mask_blocked))
    return result.reshape(SAMPLES, TASKS)
```

```python
import functools

import jax
import jax.numpy as jnp
from jax import lax
from jax.experimental import pallas as pl
from jax.experimental.pallas import tpu as pltpu
from jax.sharding import PartitionSpec as P

MESH = pl.DeviceIdType.MESH
LANES = 128
PIECE_ROWS = 64
LAG = 3
SLOT_TASKS = 14


def split_of_group(group, peers, weight_bytes, sample_bytes):
    sizes = [f for f in range(1, group + 1) if group % f == 0]

    def cost(f):
        return (f - 1) * weight_bytes + (group // f * peers - 1) * sample_bytes / 2

    return min(sizes, key=cost)


def crosses(outer, pieces, a, aa, h):
    if a == aa:
        return False
    ends = (aa == 0 and a == 1 or aa == outer - 1 and a == outer - 2) and 0 < a < outer - 1
    return ends or h == pieces - 1


def plan(outer, pieces):
    avail = [{(a, 0, h): 0 for h in range(pieces)} for a in range(outer)]
    sends = [{} for _ in range(outer)]
    arrivals = [{} for _ in range(outer)]
    done = set()
    slot = 0
    while any(len(have) < outer * pieces * 2 for have in avail):
        moves = []
        for a in range(outer):
            ends = a in (0, outer - 1)
            for way, to in ((0, a + 1), (1, a - 1)):
                if not 0 <= to < outer:
                    continue
                ready = [
                    (k, -abs(aa - a) if k else abs(aa - a), h, (aa, k, h))
                    for (aa, k, h), since in avail[a].items()
                    if since <= slot
                    and (a, way, aa, k, h) not in done
                    and (aa <= a if way == 0 else aa >= a)
                    and (k == 0 or crosses(outer, pieces, to, aa, h))
                ]
                if ready:
                    moves.append((a, way, to, min(ready)[-1]))
            ready = [
                (ends and abs(aa - a) == 1 and h == pieces - 2, since, abs(aa - a), h, (aa, 0, h))
                for (aa, k, h), since in avail[a].items()
                if since <= slot
                and k == 0
                and (a, 2, aa, k, h) not in done
                and not crosses(outer, pieces, a, aa, h)
            ]
            if ready:
                moves.append((a, 2, a, min(ready)[-1]))
        for a, way, to, (aa, k, h) in moves:
            done.add((a, way, aa, k, h))
            sends[a].setdefault((slot, way), (aa, k, h))
            got = (aa, 1 if way == 2 else k, h)
            avail[to][got] = slot + LAG
            arrivals[to].setdefault(slot, []).append(got)
        slot += 1
    return slot, sends, arrivals, avail


def tasks_of(outer, ys, pieces, towers, ready_far, avail):
    per = LANES // PIECE_ROWS
    orders = []
    for a in range(outer):
        groups = []
        for aa in range(outer):
            for k in range(ys):
                for q in range(pieces // per):
                    at = max(avail[a][aa, min(k, 1), h] for h in range(q * per, (q + 1) * per))
                    groups.append((max(at, 1), abs(aa - a), k, q, aa))
        orders.append(sorted(groups))
    count = len(orders[0])
    at = [max(orders[a][u][0] for a in range(outer)) for u in range(count)]
    at = [max(at[: u + 1]) for u in range(count)]
    last = at[-1]
    own = [[u for u in range(count) if at[u] == s] for s in range(last + 1)]
    far = []
    left = [(u, t) for t in range(towers) for u in range(count)]
    for s in range(last + 1):
        room = 10**6 if s == last else SLOT_TASKS - towers * len(own[s])
        now = [(u, t) for (u, t) in left if at[u] <= s and min(ready_far[t], last) <= s][: max(room, 0)]
        far.append(now)
        left = [x for x in left if x not in now]
    assert not left
    return [[(aa, k, q) for _, _, k, q, aa in order] for order in orders], own, far


def kernel(
    outer, inner, peers,
    feat_ref, weight_ref, bias_ref, head_ref, hbias_ref, out_ref,
    x_buf, w_buf, b_buf, c_buf, part, ret,
    load_x, load_sem, x_recv, z_send, y_send, core_send, w_send, w_recv, b_send, b_recv,
    p_send, p_recv,
):
    rows, depth = feat_ref.shape
    towers, hidden, _ = weight_ref.shape
    piece = PIECE_ROWS
    pieces = rows // piece
    per = LANES // piece
    quads = rows // LANES
    ys = peers // 2
    group_at, me = lax.axis_index("group"), lax.axis_index("peer")
    a, i = group_at // inner, group_at % inner
    y, c = me // 2, me % 2
    partner = y * 2 + (1 - c)

    def dev(a_to, i_to, p_to):
        return (a_to * inner + i_to, p_to)

    def sel(values):
        out = values[-1]
        for at in range(outer - 2, -1, -1):
            if not isinstance(out, int) or values[at] != out:
                out = jnp.where(a == at, values[at], out)
        return out

    def when(flags, do):
        if all(flags):
            do()
        elif any(flags):
            pl.when(sel([int(f) for f in flags]) == 1)(do)

    loads = [
        pltpu.make_async_copy(
            feat_ref.at[pl.ds(q * LANES, LANES)], x_buf.at[a, y, q, c], load_x.at[q]
        )
        for q in range(quads)
    ]
    load_w = pltpu.make_async_copy(weight_ref, w_buf.at[i], load_sem.at[0])
    load_b = pltpu.make_async_copy(bias_ref, b_buf.at[i, 0], load_sem.at[1])
    load_h = pltpu.make_async_copy(head_ref, b_buf.at[i, 1], load_sem.at[2])
    for load in loads:
        load.start()
    load_w.start()
    load_b.start()
    load_h.start()

    barrier = pltpu.get_barrier_semaphore()

    def greet(to):
        pl.semaphore_signal(barrier, inc=1, device_id=to, device_id_type=MESH)

    pl.when(a + 1 < outer)(lambda: greet(dev(lax.rem(a + 1, outer), i, me)))
    pl.when(a > 0)(lambda: greet(dev(lax.rem(a + outer - 1, outer), i, me)))
    for k in range(1, ys):
        greet(dev(a, i, lax.rem(y + k, ys) * 2 + c))
    for k in range(1, inner):
        greet(dev(a, lax.rem(i + k, inner), me))
    greet(dev(a, i, partner))
    neighbours = sel([(at > 0) + (at + 1 < outer) + ys + inner - 1 for at in range(outer)])

    def column(k):
        return lax.rem(y + k, ys) if k else y

    def send_x(aa, yy, cc, h, sem, to):
        ref = x_buf.at[aa, yy, h // per, cc, pl.ds(pl.multiple_of(h % per * piece, piece), piece)]
        return pltpu.make_async_remote_copy(
            src_ref=ref, dst_ref=ref, send_sem=sem, recv_sem=x_recv.at[aa, yy * 2 + cc, h],
            device_id=to, device_id_type=MESH,
        )

    def along(way, aa, k, h):
        to = lax.rem(a + 1, outer) if way == 0 else lax.rem(a + outer - 1, outer)
        return send_x(aa, column(k), c, h, z_send.at[way, aa, k, h], dev(to, i, me))

    def across(aa, k, h):
        to = dev(a, i, lax.rem(y + k, ys) * 2 + c)
        return send_x(aa, y, c, h, y_send.at[aa, k - 1, h], to)

    def sibling(aa, k, h):
        return send_x(aa, column(k), c, h, core_send.at[aa, k, h], dev(a, i, partner))

    def arrived(aa, k, cc, h):
        send_x(aa, column(k), cc, h, core_send.at[aa, k, h], dev(a, i, partner)).wait_recv()

    def send_w(k, t):
        return pltpu.make_async_remote_copy(
            src_ref=w_buf.at[i, t], dst_ref=w_buf.at[i, t],
            send_sem=w_send.at[k - 1, t], recv_sem=w_recv.at[i, t],
            device_id=dev(a, lax.rem(i + k, inner), me), device_id_type=MESH,
        )

    def send_b(k):
        return pltpu.make_async_remote_copy(
            src_ref=b_buf.at[i], dst_ref=b_buf.at[i],
            send_sem=b_send.at[k - 1], recv_sem=b_recv.at[i],
            device_id=dev(a, lax.rem(i + k, inner), me), device_id_type=MESH,
        )

    def columns(ii):
        diagonal = lax.broadcasted_iota(jnp.int32, (hidden, hidden), 0) == (
            lax.broadcasted_iota(jnp.int32, (hidden, hidden), 1)
        )
        for w in range(2):
            both = b_buf[ii, w].astype(jnp.float32)
            for t in range(towers):
                picked = jnp.where(diagonal, both[t : t + 1], 0.0)
                total = jnp.sum(picked, axis=1, keepdims=True)
                c_buf[ii, w, t] = jnp.broadcast_to(total, (hidden, LANES))

    def compute(group, ii, t, first):
        aa, yy, q = group
        x = x_buf[aa, yy, q].reshape(2 * LANES, depth)
        pre = lax.dot_general(
            w_buf[ii, t], x, (((1,), (1,)), ((), ())), preferred_element_type=jnp.float32
        )
        bias, head = c_buf[ii, 0, t], c_buf[ii, 1, t]
        lanes = pl.ds(pl.multiple_of(q * LANES, LANES), LANES)
        for cc in range(2):
            v = jnp.maximum(pre[:, cc * LANES : (cc + 1) * LANES] + bias, 0.0) * head
            total = jnp.sum(v, axis=0, keepdims=True)
            if first:
                total += jnp.where(a == 0, hbias_ref[t], 0.0)
            else:
                total += part[aa, yy * 2 + cc, pl.ds(t, 1), lanes]
            part[aa, yy * 2 + cc, pl.ds(t, 1), lanes] = total

    def send_part(aa, pp):
        return pltpu.make_async_remote_copy(
            src_ref=part.at[aa, pp], dst_ref=ret.at[a, me],
            send_sem=p_send.at[aa, pp], recv_sem=p_recv.at[a, me],
            device_id=dev(aa, i, pp), device_id_type=MESH,
        )

    def give_back(aa, yy):
        for cc in range(2):
            pp = yy * 2 + cc
            mine = (aa == a) & (pp == me)
            pl.when(jnp.logical_not(mine))(lambda pp=pp: send_part(aa, pp).start())

    slots, sends, arrivals, avail = plan(outer, pieces)
    ready_far = [-(-hidden * max(inner - 1, 1) * (t + 1) // piece) + 2 for t in range(towers)]
    orders, own, far = tasks_of(outer, ys, pieces, towers, ready_far, avail)
    steps = len(own)
    settled = [set() for _ in range(outer)]
    done_at = {}
    for s in range(steps):
        for u in own[s]:
            done_at[u] = s
        for u, _ in far[s]:
            done_at[u] = s

    def group_of(u):
        aa = sel([orders[at][u][0] for at in range(outer)])
        k = sel([orders[at][u][1] for at in range(outer)])
        q = sel([orders[at][u][2] for at in range(outer)])
        return aa, (lax.rem(y + k, ys) if not isinstance(k, int) or k else y), q

    def start_sends(slot):
        for way in range(3):
            entries = [sends[at].get((slot, way)) for at in range(outer)]
            flags = [e is not None for e in entries]
            if not any(flags):
                continue
            some = next(e for e in entries if e is not None)
            entries = [e or some for e in entries]
            issue_sends(way, entries, flags, True)

    def issue_sends(way, entries, flags, start):
        aa = sel([e[0] for e in entries])
        h = sel([e[2] for e in entries])
        kinds = sorted({e[1] for e, f in zip(entries, flags) if f})

        for kind in kinds:

            def go(kind=kind):
                for k in range(1, ys) if way == 2 or kind else (0,):
                    copy = across(aa, k, h) if way == 2 else along(way, aa, k, h)
                    copy.start() if start else copy.wait_send()

            when([f and e[1] == kind for e, f in zip(entries, flags)], go)

    def take(slot):
        lists = [arrivals[at].get(slot, []) for at in range(outer)]
        for n in range(max(len(x) for x in lists)):
            for kind in range(2):
                flags = [len(x) > n and x[n][1] == kind for x in lists]
                if not any(flags):
                    continue
                some = next(x[n] for x, f in zip(lists, flags) if f)
                entries = [x[n] if f else some for x, f in zip(lists, flags)]
                aa = sel([e[0] for e in entries])
                h = sel([e[2] for e in entries])

                def relay(aa=aa, h=h, kind=kind):
                    for k in range(1, ys) if kind else (0,):
                        arrived(aa, k, c, h)
                        sibling(aa, k, h).start()

                when(flags, relay)

    def settle(u):
        aa = sel([orders[at][u][0] for at in range(outer)])
        k = sel([orders[at][u][1] for at in range(outer)])
        q = sel([orders[at][u][2] for at in range(outer)])
        yy = lax.rem(y + k, ys)
        for n in range(per):
            ref = x_buf.at[aa, yy, q, 1 - c, pl.ds(n * piece, piece)]
            pltpu.make_async_remote_copy(
                src_ref=ref, dst_ref=ref, send_sem=core_send.at[aa, k, q * per + n],
                recv_sem=x_recv.at[aa, yy * 2 + 1 - c, q * per + n],
                device_id=dev(a, i, partner), device_id_type=MESH,
            ).wait_recv()

    def weights_arrived(t):
        for k in range(1, inner):
            ii = lax.rem(i + k, inner)
            pltpu.make_async_remote_copy(
                src_ref=w_buf.at[ii, t], dst_ref=w_buf.at[ii, t], send_sem=w_send.at[0, t],
                recv_sem=w_recv.at[ii, t], device_id=dev(a, ii, me), device_id_type=MESH,
            ).wait_recv()

    def biases_arrived():
        for k in range(1, inner):
            ii = lax.rem(i + k, inner)
            pltpu.make_async_remote_copy(
                src_ref=b_buf.at[ii], dst_ref=b_buf.at[ii], send_sem=b_send.at[0],
                recv_sem=b_recv.at[ii], device_id=dev(a, ii, me), device_id_type=MESH,
            ).wait_recv()
            columns(ii)

    pl.semaphore_wait(barrier, neighbours)
    for q, load in enumerate(loads):
        load.wait()
        if q == 0:
            start_sends(0)
            start_sends(1)
        for h in range(q * per, (q + 1) * per):
            sibling(a, 0, h).start()
    load_b.wait()
    load_h.wait()
    for k in range(1, inner):
        send_b(k).start()
    load_w.wait()
    for t in range(towers):
        for k in range(1, inner):
            send_w(k, t).start()
    columns(i)

    weights = set()
    for s in range(1, steps):
        take(s - 2)
        start_sends(s + 1)
        if s == 2:
            biases_arrived()
        for u in own[s]:
            settle(u)
            group = group_of(u)
            for t in range(towers):
                compute(group, i, t, True)
        for u, t in far[s]:
            if t not in weights:
                weights.add(t)
                weights_arrived(t)
            group = group_of(u)
            if inner == 2:
                compute(group, lax.rem(i + 1, inner), t, False)
            elif inner > 2:

                def each(k, _, group=group, t=t):
                    compute(group, lax.rem(i + k, inner), t, False)
                    return 0

                lax.fori_loop(1, inner, each, 0)
        ended = []
        for at in range(outer):
            pairs = {}
            for u, (aa, k, q) in enumerate(orders[at]):
                pairs.setdefault((aa, k), []).append(done_at[u])
            ended.append(sorted(p for p, when_done in pairs.items() if max(when_done) == s))
        for n in range(max(len(x) for x in ended)):
            flags = [len(x) > n for x in ended]
            some = next(x[n] for x in ended if len(x) > n)
            entries = [x[n] if len(x) > n else some for x in ended]
            aa = sel([e[0] for e in entries])
            k = sel([e[1] for e in entries])
            when(flags, lambda: give_back(aa, lax.rem(y + k, ys)))

    def landed(aa, pp):
        pltpu.make_async_remote_copy(
            src_ref=part.at[aa, pp], dst_ref=ret.at[aa, pp], send_sem=p_send.at[aa, pp],
            recv_sem=p_recv.at[aa, pp], device_id=dev(a, i, partner), device_id_type=MESH,
        ).wait_recv()

    for slot in range(slots):
        for way in range(3):
            entries = [sends[at].get((slot, way)) for at in range(outer)]
            flags = [e is not None for e in entries]
            if any(flags):
                some = next(e for e in entries if e is not None)
                issue_sends(way, [e or some for e in entries], flags, False)
    for aa in range(outer):
        for k in range(ys):
            for h in range(pieces):
                sibling(aa, k, h).wait_send()
    for k in range(1, inner):
        send_b(k).wait_send()
        for t in range(towers):
            send_w(k, t).wait_send()

    ret[a, me] = part[a, me]
    for aa in range(outer):
        for pp in range(peers):
            mine = (a == aa) & (me == pp)
            pl.when(jnp.logical_not(mine))(lambda aa=aa, pp=pp: landed(aa, pp))
    for pp in range(peers):
        total = ret[0, pp]
        for aa in range(1, outer):
            total += ret[aa, pp]
        out_ref[pp * towers : (pp + 1) * towers] = total
    for aa in range(outer):
        for pp in range(peers):
            mine = (a == aa) & (me == pp)
            pl.when(jnp.logical_not(mine))(lambda aa=aa, pp=pp: send_part(aa, pp).wait_send())


def shards(features, task_mask, tower_in, tower_bias, tower_head, head_bias):
    peers, group = lax.axis_size("peer"), lax.axis_size("group")
    rows, depth = features.shape
    towers, hidden, _ = tower_in.shape
    inner = split_of_group(group, peers, tower_in.size, features.size)
    outer = group // inner
    ys = peers // 2
    pieces = rows // PIECE_ROWS
    dma = pltpu.SemaphoreType.DMA
    logits = pl.pallas_call(
        functools.partial(kernel, outer, inner, peers),
        out_shape=jax.ShapeDtypeStruct((peers * towers, rows), jnp.float32),
        in_specs=[pl.BlockSpec(memory_space=pl.ANY)] * 4
        + [pl.BlockSpec(memory_space=pltpu.SMEM)],
        out_specs=pl.BlockSpec(memory_space=pltpu.VMEM),
        scratch_shapes=[
            pltpu.VMEM((outer, ys, rows // LANES, 2, LANES, depth), features.dtype),
            pltpu.VMEM((inner, towers, hidden, depth), tower_in.dtype),
            pltpu.VMEM((inner, 2, towers, hidden), tower_bias.dtype),
            pltpu.VMEM((inner, 2, towers, hidden, LANES), jnp.float32),
            pltpu.VMEM((outer, peers, towers, rows), jnp.float32),
            pltpu.VMEM((outer, peers, towers, rows), jnp.float32),
            dma((rows // LANES,)),
            dma((3,)),
            dma((outer, peers, pieces)),
            dma((2, outer, ys, pieces)),
            dma((outer, max(1, ys - 1), pieces)),
            dma((outer, ys, pieces)),
            dma((max(1, inner - 1), towers)),
            dma((inner, towers)),
            dma((max(1, inner - 1),)),
            dma((inner,)),
            dma((outer, peers)),
            dma((outer, peers)),
        ],
        compiler_params=pltpu.CompilerParams(
            collective_id=0, has_side_effects=True, vmem_limit_bytes=60 * 1024 * 1024
        ),
    )(features, tower_in, tower_bias, tower_head, head_bias)
    tasks = jnp.arange(peers * towers, dtype=jnp.int32)
    bits = (task_mask[:, None] >> tasks[None, :]) & 1
    return jnp.where(bits == 1, logits.T, 0.0)


def solution(mesh):
    placed = (
        P(("group", "peer"), None),
        P(("group", "peer")),
        P("peer", "group", None),
        P("peer", "group"),
        P("peer", "group"),
        P("peer"),
    )
    return jax.shard_map(
        shards, mesh=mesh, in_specs=placed, out_specs=P(("group", "peer"), None), check_vma=False
    )
```

```python
import functools

import jax
import jax.numpy as jnp
from jax import lax
from jax.experimental import pallas as pl
from jax.experimental.pallas import tpu as pltpu
from jax.sharding import PartitionSpec as P

MESH = pl.DeviceIdType.MESH
LANES = 128
PIECE_ROWS = 64
LAG = 3
SLOT_TASKS = 14


def split_of_group(group, peers, weight_bytes, sample_bytes):
    sizes = [f for f in range(1, group + 1) if group % f == 0]

    def cost(f):
        return (f - 1) * weight_bytes + (group // f * peers - 1) * sample_bytes / 2

    return min(sizes, key=cost)


def crosses(outer, pieces, a, aa, h):
    if a == aa:
        return False
    ends = (aa == 0 and a == 1 or aa == outer - 1 and a == outer - 2) and 0 < a < outer - 1
    return ends or h == pieces - 1


def plan(outer, pieces):
    avail = [{(a, 0, h): 0 for h in range(pieces)} for a in range(outer)]
    sends = [{} for _ in range(outer)]
    arrivals = [{} for _ in range(outer)]
    done = set()
    slot = 0
    while any(len(have) < outer * pieces * 2 for have in avail):
        moves = []
        for a in range(outer):
            ends = a in (0, outer - 1)
            for way, to in ((0, a + 1), (1, a - 1)):
                if not 0 <= to < outer:
                    continue
                ready = [
                    (k, k and abs(aa - to) == 1, abs(aa - to), h, (aa, k, h))
                    for (aa, k, h), since in avail[a].items()
                    if since <= slot
                    and (a, way, aa, k, h) not in done
                    and (aa <= a if way == 0 else aa >= a)
                    and (k == 0 or crosses(outer, pieces, to, aa, h))
                ]
                if ready:
                    moves.append((a, way, to, min(ready)[-1]))
            ready = [
                (ends and abs(aa - a) == 1 and h == pieces - 2, since, abs(aa - a), h, (aa, 0, h))
                for (aa, k, h), since in avail[a].items()
                if since <= slot
                and k == 0
                and (a, 2, aa, k, h) not in done
                and not crosses(outer, pieces, a, aa, h)
            ]
            if ready:
                moves.append((a, 2, a, min(ready)[-1]))
        for a, way, to, (aa, k, h) in moves:
            done.add((a, way, aa, k, h))
            sends[a].setdefault((slot, way), (aa, k, h))
            got = (aa, 1 if way == 2 else k, h)
            avail[to][got] = slot + LAG
            arrivals[to].setdefault(slot, []).append((*got, way))
        slot += 1
    return slot, sends, arrivals, avail


def tasks_of(outer, ys, pieces, towers, ready_far, avail):
    per = LANES // PIECE_ROWS
    orders = []
    for a in range(outer):
        groups = []
        for aa in range(outer):
            for k in range(ys):
                for q in range(pieces // per):
                    at = max(avail[a][aa, min(k, 1), h] for h in range(q * per, (q + 1) * per))
                    groups.append((max(at, 1), abs(aa - a), k, q, aa))
        orders.append(sorted(groups))
    count = len(orders[0])
    at = [max(orders[a][u][0] for a in range(outer)) for u in range(count)]
    at = [max(at[: u + 1]) for u in range(count)]
    last = at[-1]
    own = [[u for u in range(count) if at[u] == s] for s in range(last + 1)]
    far = []
    left = [(u, t) for t in range(towers) for u in range(count)]
    for s in range(last + 1):
        room = 10**6 if s == last else SLOT_TASKS - towers * len(own[s])
        now = [(u, t) for (u, t) in left if at[u] <= s and min(ready_far[t], last) <= s][: max(room, 0)]
        far.append(now)
        left = [x for x in left if x not in now]
    assert not left
    return [[(aa, k, q) for _, _, k, q, aa in order] for order in orders], own, far


def kernel(
    outer, inner, peers,
    feat_ref, weight_ref, bias_ref, head_ref, hbias_ref, out_ref,
    x_buf, w_buf, b_buf, c_buf, part, ret,
    load_sem, x_recv, core_recv, x_send, core_send, w_send, w_recv, b_send, b_recv, p_send, p_recv,
):
    rows, depth = feat_ref.shape
    towers, hidden, _ = weight_ref.shape
    piece = PIECE_ROWS
    pieces = rows // piece
    per = LANES // piece
    quads = rows // LANES
    ys = peers // 2
    group_at, me = lax.axis_index("group"), lax.axis_index("peer")
    a, i = group_at // inner, group_at % inner
    y, c = me // 2, me % 2
    partner = y * 2 + (1 - c)

    def dev(a_to, i_to, p_to):
        return (a_to * inner + i_to, p_to)

    def sel(values):
        out = values[-1]
        for at in range(outer - 2, -1, -1):
            if not isinstance(out, int) or values[at] != out:
                out = jnp.where(a == at, values[at], out)
        return out

    def when(flags, do):
        if all(flags):
            do()
        elif any(flags):
            pl.when(sel([int(f) for f in flags]) == 1)(do)

    def at_group(aa, yy, q):
        return (aa * ys + yy) * quads + q

    def x_rows(aa, yy, q, cc, start=0, size=LANES):
        row = (at_group(aa, yy, q) * 2 + cc) * LANES + start
        return x_buf.at[pl.ds(pl.multiple_of(row, PIECE_ROWS), size)]

    loads = [
        pltpu.make_async_copy(
            feat_ref.at[pl.ds(q * LANES, LANES)], x_rows(a, y, q, c), load_sem.at[q]
        )
        for q in range(quads)
    ]
    load_w = pltpu.make_async_copy(weight_ref, w_buf.at[i], load_sem.at[quads])
    load_b = pltpu.make_async_copy(bias_ref, b_buf.at[i, 0], load_sem.at[quads + 1])
    load_h = pltpu.make_async_copy(head_ref, b_buf.at[i, 1], load_sem.at[quads + 2])
    for load in loads:
        load.start()
    load_w.start()
    load_b.start()
    load_h.start()

    barrier = pltpu.get_barrier_semaphore()

    def greet(to):
        pl.semaphore_signal(barrier, inc=1, device_id=to, device_id_type=MESH)

    pl.when(a + 1 < outer)(lambda: greet(dev(lax.rem(a + 1, outer), i, me)))
    pl.when(a > 0)(lambda: greet(dev(lax.rem(a + outer - 1, outer), i, me)))
    for k in range(1, ys):
        greet(dev(a, i, lax.rem(y + k, ys) * 2 + c))
    for k in range(1, inner):
        greet(dev(a, lax.rem(i + k, inner), me))
    greet(dev(a, i, partner))
    neighbours = sel([(at > 0) + (at + 1 < outer) + ys + inner - 1 for at in range(outer)])

    def column(k):
        return lax.rem(y + k, ys) if k else y

    def send_x(aa, yy, h, send_sem, recv_sem, to):
        ref = x_rows(aa, yy, h // per, c, h % per * piece, piece)
        return pltpu.make_async_remote_copy(
            src_ref=ref, dst_ref=ref, send_sem=send_sem, recv_sem=recv_sem,
            device_id=to, device_id_type=MESH,
        )

    def along(way, aa, k, h, slot):
        to = lax.rem(a + 1, outer) if way == 0 else lax.rem(a + outer - 1, outer)
        return send_x(aa, column(k), h, x_send.at[0], x_recv.at[0, slot], dev(to, i, me))

    def across(aa, k, h, slot):
        to = dev(a, i, lax.rem(y + k, ys) * 2 + c)
        return send_x(aa, y, h, x_send.at[0], x_recv.at[1, slot], to)

    def sibling(aa, k, h):
        sem = core_recv.at[at_group(aa, column(k), h // per)]
        return send_x(aa, column(k), h, core_send.at[0], sem, dev(a, i, partner))

    def await_rows(count, sem):
        ref = x_buf.at[pl.ds(0, count)]
        pltpu.make_async_remote_copy(
            src_ref=ref, dst_ref=ref, send_sem=x_send.at[0], recv_sem=sem,
            device_id=dev(a, i, partner), device_id_type=MESH,
        ).wait_recv()

    def await_sent(count, sem):
        ref = x_buf.at[pl.ds(0, count)]
        pltpu.make_async_remote_copy(
            src_ref=ref, dst_ref=ref, send_sem=sem.at[0], recv_sem=p_recv.at[0],
            device_id=dev(a, i, partner), device_id_type=MESH,
        ).wait_send()

    def send_w(k, t):
        return pltpu.make_async_remote_copy(
            src_ref=w_buf.at[i, t], dst_ref=w_buf.at[i, t], send_sem=w_send.at[0],
            recv_sem=w_recv.at[t], device_id=dev(a, lax.rem(i + k, inner), me), device_id_type=MESH,
        )

    def send_b(k):
        return pltpu.make_async_remote_copy(
            src_ref=b_buf.at[i], dst_ref=b_buf.at[i], send_sem=b_send.at[0],
            recv_sem=b_recv.at[0], device_id=dev(a, lax.rem(i + k, inner), me), device_id_type=MESH,
        )

    def await_all(ref, send_sem, recv_sem, sent):
        copy = pltpu.make_async_remote_copy(
            src_ref=ref, dst_ref=ref, send_sem=send_sem.at[0], recv_sem=recv_sem,
            device_id=dev(a, i, partner), device_id_type=MESH,
        )
        copy.wait_send() if sent else copy.wait_recv()

    def columns(ii):
        diagonal = lax.broadcasted_iota(jnp.int32, (hidden, hidden), 0) == (
            lax.broadcasted_iota(jnp.int32, (hidden, hidden), 1)
        )
        for w in range(2):
            both = b_buf[ii, w].astype(jnp.float32)
            for t in range(towers):
                picked = jnp.where(diagonal, both[t : t + 1], 0.0)
                total = jnp.sum(picked, axis=1, keepdims=True)
                c_buf[ii, w, t] = jnp.broadcast_to(total, (hidden, LANES))

    def compute(group, ii, t, first):
        aa, yy, q = group
        row = pl.multiple_of(at_group(aa, yy, q) * 2 * LANES, 2 * LANES)
        x = x_buf[pl.ds(row, 2 * LANES)]
        pre = lax.dot_general(
            w_buf[ii, t], x, (((1,), (1,)), ((), ())), preferred_element_type=jnp.float32
        )
        bias, head = c_buf[ii, 0, t], c_buf[ii, 1, t]
        lanes = pl.ds(pl.multiple_of(q * LANES, LANES), LANES)
        for cc in range(2):
            v = jnp.maximum(pre[:, cc * LANES : (cc + 1) * LANES] + bias, 0.0) * head
            total = jnp.sum(v, axis=0, keepdims=True)
            if first:
                total += jnp.where(a == 0, hbias_ref[t], 0.0)
            else:
                total += part[aa * peers + yy * 2 + cc, pl.ds(t, 1), lanes]
            part[aa * peers + yy * 2 + cc, pl.ds(t, 1), lanes] = total

    def send_part(aa, pp):
        return pltpu.make_async_remote_copy(
            src_ref=part.at[aa * peers + pp], dst_ref=ret.at[a * peers + me],
            send_sem=p_send.at[0], recv_sem=p_recv.at[0],
            device_id=dev(aa, i, pp), device_id_type=MESH,
        )

    def give_back(aa, yy):
        for cc in range(2):
            pp = yy * 2 + cc
            mine = (aa == a) & (pp == me)
            pl.when(jnp.logical_not(mine))(lambda pp=pp: send_part(aa, pp).start())

    slots, sends, arrivals, avail = plan(outer, pieces)
    ready_far = [-(-hidden * max(inner - 1, 1) * (t + 1) // piece) + 2 for t in range(towers)]
    orders, own, far = tasks_of(outer, ys, pieces, towers, ready_far, avail)
    steps = len(own)
    done_at = {}
    for s in range(steps):
        for u in own[s]:
            done_at[u] = s
        for u, _ in far[s]:
            done_at[u] = s

    def group_of(u):
        aa = sel([orders[at][u][0] for at in range(outer)])
        k = sel([orders[at][u][1] for at in range(outer)])
        q = sel([orders[at][u][2] for at in range(outer)])
        return aa, (lax.rem(y + k, ys) if not isinstance(k, int) or k else y), q

    def start_sends(slot):
        for way in range(3):
            entries = [sends[at].get((slot, way)) for at in range(outer)]
            flags = [e is not None for e in entries]
            if not any(flags):
                continue
            some = next(e for e in entries if e is not None)
            entries = [e or some for e in entries]
            issue_sends(way, entries, flags, slot)

    def issue_sends(way, entries, flags, slot):
        aa = sel([e[0] for e in entries])
        h = sel([e[2] for e in entries])
        kinds = sorted({e[1] for e, f in zip(entries, flags) if f})

        for kind in kinds:

            def go(kind=kind):
                for k in range(1, ys) if way == 2 or kind else (0,):
                    copy = across(aa, k, h, slot) if way == 2 else along(way, aa, k, h, slot)
                    copy.start()

            when([f and e[1] == kind for e, f in zip(entries, flags)], go)

    def by_count(counts, do):
        for count in sorted(set(counts) - {0}):
            when([n == count for n in counts], lambda count=count: do(count))

    def take(slot):
        lists = [arrivals[at].get(slot, []) for at in range(outer)]
        for link in range(2):
            kept = [[e for *e, way in x if (way == 2) == (link == 1)] for x in lists]
            counts = [sum(ys - 1 if k else 1 for _, k, _ in x) for x in kept]
            by_count(counts, lambda n: await_rows(n * piece, x_recv.at[link, slot]))
            for n in range(max(len(x) for x in kept)):
                for kind in range(2):
                    flags = [len(x) > n and x[n][1] == kind for x in kept]
                    if not any(flags):
                        continue
                    some = next(x[n] for x, f in zip(kept, flags) if f)
                    entries = [x[n] if f else some for x, f in zip(kept, flags)]
                    aa = sel([e[0] for e in entries])
                    h = sel([e[2] for e in entries])

                    def relay(aa=aa, h=h, kind=kind):
                        for k in range(1, ys) if kind else (0,):
                            sibling(aa, k, h).start()

                    when(flags, relay)

    def settle(u):
        await_rows(LANES, core_recv.at[at_group(*group_of(u))])

    def weights_arrived(t):
        if inner > 1:
            await_all(w_buf.at[pl.ds(0, inner - 1), t], w_send, w_recv.at[t], False)

    def biases_arrived():
        if inner > 1:
            await_all(b_buf.at[pl.ds(0, inner - 1)], b_send, b_recv.at[0], False)
        for k in range(1, inner):
            columns(lax.rem(i + k, inner))

    pl.semaphore_wait(barrier, neighbours)
    for load in loads:
        load.wait()
    start_sends(0)
    start_sends(1)
    load_b.wait()
    load_h.wait()
    for k in range(1, inner):
        send_b(k).start()
    load_w.wait()
    for t in range(towers):
        for k in range(1, inner):
            send_w(k, t).start()
    columns(i)
    for h in range(pieces):
        sibling(a, 0, h).start()

    weights = set()
    def far_tasks(s):
        for u, t in far[s]:
            if t not in weights:
                weights.add(t)
                weights_arrived(t)
            group = group_of(u)
            if inner == 2:
                compute(group, lax.rem(i + 1, inner), t, False)
            elif inner > 2:

                def each(k, _, group=group, t=t):
                    compute(group, lax.rem(i + k, inner), t, False)
                    return 0

                lax.fori_loop(1, inner, each, 0)

    for s in range(1, steps):
        for u in own[s]:
            settle(u)
            for t in range(towers):
                compute(group_of(u), i, t, True)
        if s > slots:
            far_tasks(s)
        take(s - 2)
        start_sends(s + 1)
        if s == 2:
            biases_arrived()
        if s <= slots:
            far_tasks(s)
        ended = []
        for at in range(outer):
            pairs = {}
            for u, (aa, k, q) in enumerate(orders[at]):
                pairs.setdefault((aa, k), []).append(done_at[u])
            ended.append(sorted(p for p, when_done in pairs.items() if max(when_done) == s))
        for n in range(max(len(x) for x in ended)):
            flags = [len(x) > n for x in ended]
            some = next(x[n] for x in ended if len(x) > n)
            entries = [x[n] if len(x) > n else some for x in ended]
            aa = sel([e[0] for e in entries])
            k = sel([e[1] for e in entries])
            when(flags, lambda: give_back(aa, lax.rem(y + k, ys)))

    counts = []
    for at in range(outer):
        each_way = [(ys - 1 if way == 2 or e[1] else 1) for (_, way), e in sends[at].items()]
        counts.append(sum(each_way))
    by_count(counts, lambda n: await_sent(n * piece, x_send))
    await_sent(outer * ys * pieces * piece, core_send)
    if inner > 1:
        await_all(w_buf.at[pl.ds(0, inner - 1)], w_send, w_recv.at[0], True)
        await_all(b_buf.at[pl.ds(0, inner - 1)], b_send, b_recv.at[0], True)
    ret[a * peers + me] = part[a * peers + me]
    await_all(ret.at[pl.ds(0, outer * peers - 1)], p_send, p_recv.at[0], False)
    for pp in range(peers):
        total = ret[pp]
        for aa in range(1, outer):
            total += ret[aa * peers + pp]
        out_ref[pp * towers : (pp + 1) * towers] = total
    await_all(part.at[pl.ds(0, outer * peers - 1)], p_send, p_recv.at[0], True)


def shards(features, task_mask, tower_in, tower_bias, tower_head, head_bias):
    peers, group = lax.axis_size("peer"), lax.axis_size("group")
    rows, depth = features.shape
    towers, hidden, _ = tower_in.shape
    inner = split_of_group(group, peers, tower_in.size, features.size)
    outer = group // inner
    ys = peers // 2
    pieces = rows // PIECE_ROWS
    dma = pltpu.SemaphoreType.DMA
    logits = pl.pallas_call(
        functools.partial(kernel, outer, inner, peers),
        out_shape=jax.ShapeDtypeStruct((peers * towers, rows), jnp.float32),
        in_specs=[pl.BlockSpec(memory_space=pl.ANY)] * 4
        + [pl.BlockSpec(memory_space=pltpu.SMEM)],
        out_specs=pl.BlockSpec(memory_space=pltpu.VMEM),
        scratch_shapes=[
            pltpu.VMEM((outer * peers * rows, depth), features.dtype),
            pltpu.VMEM((inner, towers, hidden, depth), tower_in.dtype),
            pltpu.VMEM((inner, 2, towers, hidden), tower_bias.dtype),
            pltpu.VMEM((inner, 2, towers, hidden, LANES), jnp.float32),
            pltpu.VMEM((outer * peers, towers, rows), jnp.float32),
            pltpu.VMEM((outer * peers, towers, rows), jnp.float32),
            dma((rows // LANES + 3,)),
            dma((2, plan(outer, pieces)[0])),
            dma((outer * ys * rows // LANES,)),
            dma((1,)),
            dma((1,)),
            dma((1,)),
            dma((towers,)),
            dma((1,)),
            dma((1,)),
            dma((1,)),
            dma((1,)),
        ],
        compiler_params=pltpu.CompilerParams(
            collective_id=0, has_side_effects=True, vmem_limit_bytes=60 * 1024 * 1024
        ),
    )(features, tower_in, tower_bias, tower_head, head_bias)
    tasks = jnp.arange(peers * towers, dtype=jnp.int32)
    bits = (task_mask[:, None] >> tasks[None, :]) & 1
    return jnp.where(bits == 1, logits.T, 0.0)


def solution(mesh):
    placed = (
        P(("group", "peer"), None),
        P(("group", "peer")),
        P("peer", "group", None),
        P("peer", "group"),
        P("peer", "group"),
        P("peer"),
    )
    return jax.shard_map(
        shards, mesh=mesh, in_specs=placed, out_specs=P(("group", "peer"), None), check_vma=False
    )
```

```python
import functools

import jax
import jax.numpy as jnp
from jax import lax
from jax.experimental import pallas as pl
from jax.experimental.pallas import tpu as pltpu
from jax.sharding import PartitionSpec as P

MESH = pl.DeviceIdType.MESH
LANES = 128
PIECE_ROWS = 64
LAG = 3
SLOT_TASKS = 16


def split_of_group(group, peers, weight_bytes, sample_bytes):
    sizes = [f for f in range(1, group + 1) if group % f == 0]

    def cost(f):
        return (f - 1) * weight_bytes + (group // f * peers - 1) * sample_bytes / 2

    return min(sizes, key=cost)


def crosses(outer, pieces, a, aa, h):
    if a == aa:
        return False
    ends = (aa == 0 and a == 1 or aa == outer - 1 and a == outer - 2) and 0 < a < outer - 1
    return ends or h == pieces - 1


def plan(outer, pieces):
    def late(a, aa, h):
        held = a in (0, outer - 1) and h == pieces - 2 and abs(aa - a) in (1, 2)
        return held, -abs(aa - a) if held else 0

    avail = [{(a, 0, h): 0 for h in range(pieces)} for a in range(outer)]
    sends = [{} for _ in range(outer)]
    arrivals = [{} for _ in range(outer)]
    done = set()
    slot = 0
    while any(len(have) < outer * pieces * 2 for have in avail):
        moves = []
        for a in range(outer):
            for way, to in ((0, a + 1), (1, a - 1)):
                if not 0 <= to < outer:
                    continue
                ready = [
                    (k, -abs(aa - to), h, (aa, k, h))
                    for (aa, k, h), since in avail[a].items()
                    if since <= slot
                    and (a, way, aa, k, h) not in done
                    and (aa <= a if way == 0 else aa >= a)
                    and (k == 0 or crosses(outer, pieces, to, aa, h))
                ]
                if ready:
                    moves.append((a, way, to, min(ready)[-1]))
            ready = [
                (*late(a, aa, h), since, h, (aa, 0, h))
                for (aa, k, h), since in avail[a].items()
                if since <= slot
                and k == 0
                and (a, 2, aa, k, h) not in done
                and not crosses(outer, pieces, a, aa, h)
            ]
            if ready:
                moves.append((a, 2, a, min(ready)[-1]))
        for a, way, to, (aa, k, h) in moves:
            done.add((a, way, aa, k, h))
            sends[a].setdefault((slot, way), (aa, k, h))
            got = (aa, 1 if way == 2 else k, h)
            avail[to][got] = slot + LAG
            arrivals[to].setdefault(slot, []).append((*got, way))
        slot += 1
    return slot, sends, arrivals, avail


def tasks_of(outer, ys, pieces, towers, ready_far, avail):
    per = LANES // PIECE_ROWS
    orders = []
    for a in range(outer):
        groups = []
        for aa in range(outer):
            for k in range(ys):
                for q in range(pieces // per):
                    at = max(avail[a][aa, min(k, 1), h] for h in range(q * per, (q + 1) * per))
                    groups.append((max(at, 1), abs(aa - a), k, q, aa))
        orders.append(sorted(groups))
    count = len(orders[0])
    at = [max(orders[a][u][0] for a in range(outer)) for u in range(count)]
    at = [max(at[: u + 1]) for u in range(count)]
    last = at[-1]
    own = [[u for u in range(count) if at[u] == s] for s in range(last + 1)]
    far = []
    left = [(u, t) for t in range(towers) for u in range(count)]
    for s in range(last + 1):
        room = 10**6 if s == last else SLOT_TASKS - towers * len(own[s])
        now = [(u, t) for (u, t) in left if at[u] <= s and min(ready_far[t], last) <= s][: max(room, 0)]
        far.append(now)
        left = [x for x in left if x not in now]
    assert not left
    return [[(aa, k, q) for _, _, k, q, aa in order] for order in orders], own, far


def kernel(
    outer, inner, peers,
    feat_ref, weight_ref, bias_ref, head_ref, hbias_ref, out_ref,
    x_buf, w_buf, b_buf, c_buf, part, ret,
    load_sem, x_recv, core_recv, x_send, core_send, w_send, w_recv, b_send, b_recv, p_send, p_recv,
):
    rows, depth = feat_ref.shape
    towers, hidden, _ = weight_ref.shape
    piece = PIECE_ROWS
    pieces = rows // piece
    per = LANES // piece
    quads = rows // LANES
    ys = peers // 2
    group_at, me = lax.axis_index("group"), lax.axis_index("peer")
    a, i = group_at // inner, group_at % inner
    y, c = me // 2, me % 2
    partner = y * 2 + (1 - c)

    def dev(a_to, i_to, p_to):
        return (a_to * inner + i_to, p_to)

    def sel(values):
        out = values[-1]
        for at in range(outer - 2, -1, -1):
            if not isinstance(out, int) or values[at] != out:
                out = jnp.where(a == at, values[at], out)
        return out

    def when(flags, do):
        if all(flags):
            do()
        elif any(flags):
            pl.when(sel([int(f) for f in flags]) == 1)(do)

    def at_group(aa, yy, q):
        return (aa * ys + yy) * quads + q

    def x_rows(aa, yy, q, cc, start=0, size=LANES):
        row = (at_group(aa, yy, q) * 2 + cc) * LANES + start
        return x_buf.at[pl.ds(pl.multiple_of(row, PIECE_ROWS), size)]

    loads = [
        pltpu.make_async_copy(
            feat_ref.at[pl.ds(q * LANES, LANES)], x_rows(a, y, q, c), load_sem.at[q]
        )
        for q in range(quads)
    ]
    load_w = pltpu.make_async_copy(weight_ref, w_buf.at[i], load_sem.at[quads])
    load_b = pltpu.make_async_copy(bias_ref, b_buf.at[i, 0], load_sem.at[quads + 1])
    load_h = pltpu.make_async_copy(head_ref, b_buf.at[i, 1], load_sem.at[quads + 2])
    barrier = pltpu.get_barrier_semaphore()

    def greet(to):
        pl.semaphore_signal(barrier, inc=1, device_id=to, device_id_type=MESH)

    pl.when(a + 1 < outer)(lambda: greet(dev(lax.rem(a + 1, outer), i, me)))
    pl.when(a > 0)(lambda: greet(dev(lax.rem(a + outer - 1, outer), i, me)))
    for k in range(1, ys):
        greet(dev(a, i, lax.rem(y + k, ys) * 2 + c))
    for k in range(1, inner):
        greet(dev(a, lax.rem(i + k, inner), me))
    greet(dev(a, i, partner))
    for load in loads:
        load.start()
    load_w.start()
    load_b.start()
    load_h.start()
    neighbours = sel([(at > 0) + (at + 1 < outer) + ys + inner - 1 for at in range(outer)])

    def column(k):
        return lax.rem(y + k, ys) if k else y

    def send_x(aa, yy, h, send_sem, recv_sem, to):
        ref = x_rows(aa, yy, h // per, c, h % per * piece, piece)
        return pltpu.make_async_remote_copy(
            src_ref=ref, dst_ref=ref, send_sem=send_sem, recv_sem=recv_sem,
            device_id=to, device_id_type=MESH,
        )

    def along(way, aa, k, h, slot):
        to = lax.rem(a + 1, outer) if way == 0 else lax.rem(a + outer - 1, outer)
        return send_x(aa, column(k), h, x_send.at[0], x_recv.at[0, slot], dev(to, i, me))

    def across(aa, k, h, slot):
        to = dev(a, i, lax.rem(y + k, ys) * 2 + c)
        return send_x(aa, y, h, x_send.at[0], x_recv.at[1, slot], to)

    def sibling(aa, k, h):
        sem = core_recv.at[at_group(aa, column(k), h // per)]
        return send_x(aa, column(k), h, core_send.at[0], sem, dev(a, i, partner))

    def await_rows(count, sem):
        ref = x_buf.at[pl.ds(0, count)]
        pltpu.make_async_remote_copy(
            src_ref=ref, dst_ref=ref, send_sem=x_send.at[0], recv_sem=sem,
            device_id=dev(a, i, partner), device_id_type=MESH,
        ).wait_recv()

    def await_sent(count, sem):
        ref = x_buf.at[pl.ds(0, count)]
        pltpu.make_async_remote_copy(
            src_ref=ref, dst_ref=ref, send_sem=sem.at[0], recv_sem=p_recv.at[0],
            device_id=dev(a, i, partner), device_id_type=MESH,
        ).wait_send()

    def send_w(k, t):
        return pltpu.make_async_remote_copy(
            src_ref=w_buf.at[i, t], dst_ref=w_buf.at[i, t], send_sem=w_send.at[0],
            recv_sem=w_recv.at[t], device_id=dev(a, lax.rem(i + k, inner), me), device_id_type=MESH,
        )

    def send_b(k):
        return pltpu.make_async_remote_copy(
            src_ref=b_buf.at[i], dst_ref=b_buf.at[i], send_sem=b_send.at[0],
            recv_sem=b_recv.at[0], device_id=dev(a, lax.rem(i + k, inner), me), device_id_type=MESH,
        )

    def await_all(ref, send_sem, recv_sem, sent):
        copy = pltpu.make_async_remote_copy(
            src_ref=ref, dst_ref=ref, send_sem=send_sem.at[0], recv_sem=recv_sem,
            device_id=dev(a, i, partner), device_id_type=MESH,
        )
        copy.wait_send() if sent else copy.wait_recv()

    def columns(ii):
        diagonal = lax.broadcasted_iota(jnp.int32, (hidden, hidden), 0) == (
            lax.broadcasted_iota(jnp.int32, (hidden, hidden), 1)
        )
        for w in range(2):
            both = b_buf[ii, w].astype(jnp.float32)
            for t in range(towers):
                picked = jnp.where(diagonal, both[t : t + 1], 0.0)
                total = jnp.sum(picked, axis=1, keepdims=True)
                c_buf[ii, w, t] = jnp.broadcast_to(total, (hidden, LANES))

    def compute(group, ii, t, first):
        aa, yy, q = group
        row = pl.multiple_of(at_group(aa, yy, q) * 2 * LANES, 2 * LANES)
        x = x_buf[pl.ds(row, 2 * LANES)]
        pre = lax.dot_general(
            w_buf[ii, t], x, (((1,), (1,)), ((), ())), preferred_element_type=jnp.float32
        )
        bias, head = c_buf[ii, 0, t], c_buf[ii, 1, t]
        lanes = pl.ds(pl.multiple_of(q * LANES, LANES), LANES)
        for cc in range(2):
            v = jnp.maximum(pre[:, cc * LANES : (cc + 1) * LANES] + bias, 0.0) * head
            total = jnp.sum(v, axis=0, keepdims=True)
            if first:
                total += jnp.where(a == 0, hbias_ref[t], 0.0)
            else:
                total += part[aa * peers + yy * 2 + cc, pl.ds(t, 1), lanes]
            part[aa * peers + yy * 2 + cc, pl.ds(t, 1), lanes] = total

    def send_part(aa, pp):
        return pltpu.make_async_remote_copy(
            src_ref=part.at[aa * peers + pp], dst_ref=ret.at[a * peers + me],
            send_sem=p_send.at[0], recv_sem=p_recv.at[0],
            device_id=dev(aa, i, pp), device_id_type=MESH,
        )

    def give_back(aa, yy):
        for cc in range(2):
            pp = yy * 2 + cc
            mine = (aa == a) & (pp == me)
            pl.when(jnp.logical_not(mine))(lambda pp=pp: send_part(aa, pp).start())

    slots, sends, arrivals, avail = plan(outer, pieces)
    ready_far = [-(-hidden * max(inner - 1, 1) * (t + 1) // piece) + 1 for t in range(towers)]
    orders, own, far = tasks_of(outer, ys, pieces, towers, ready_far, avail)
    steps = len(own)
    done_at = {}
    for s in range(steps):
        for u in own[s]:
            done_at[u] = s
        for u, _ in far[s]:
            done_at[u] = s

    def group_of(u):
        aa = sel([orders[at][u][0] for at in range(outer)])
        k = sel([orders[at][u][1] for at in range(outer)])
        q = sel([orders[at][u][2] for at in range(outer)])
        return aa, (lax.rem(y + k, ys) if not isinstance(k, int) or k else y), q

    def start_sends(slot):
        for way in range(3):
            entries = [sends[at].get((slot, way)) for at in range(outer)]
            flags = [e is not None for e in entries]
            if not any(flags):
                continue
            some = next(e for e in entries if e is not None)
            entries = [e or some for e in entries]
            issue_sends(way, entries, flags, slot)

    def issue_sends(way, entries, flags, slot):
        aa = sel([e[0] for e in entries])
        h = sel([e[2] for e in entries])
        kinds = sorted({e[1] for e, f in zip(entries, flags) if f})

        for kind in kinds:

            def go(kind=kind):
                for k in range(1, ys) if way == 2 or kind else (0,):
                    copy = across(aa, k, h, slot) if way == 2 else along(way, aa, k, h, slot)
                    copy.start()

            when([f and e[1] == kind for e, f in zip(entries, flags)], go)

    def by_count(counts, do):
        for count in sorted(set(counts) - {0}):
            when([n == count for n in counts], lambda count=count: do(count))

    def take(slot):
        lists = [arrivals[at].get(slot, []) for at in range(outer)]
        for link in range(2):
            kept = [[e for *e, way in x if (way == 2) == (link == 1)] for x in lists]
            counts = [sum(ys - 1 if k else 1 for _, k, _ in x) for x in kept]
            by_count(counts, lambda n: await_rows(n * piece, x_recv.at[link, slot]))
            for n in range(max(len(x) for x in kept)):
                for kind in range(2):
                    flags = [len(x) > n and x[n][1] == kind for x in kept]
                    if not any(flags):
                        continue
                    some = next(x[n] for x, f in zip(kept, flags) if f)
                    entries = [x[n] if f else some for x, f in zip(kept, flags)]
                    aa = sel([e[0] for e in entries])
                    h = sel([e[2] for e in entries])

                    def relay(aa=aa, h=h, kind=kind):
                        for k in range(1, ys) if kind else (0,):
                            sibling(aa, k, h).start()

                    when(flags, relay)

    def settle(u):
        await_rows(LANES, core_recv.at[at_group(*group_of(u))])

    def weights_arrived(t):
        if inner > 1:
            await_all(w_buf.at[pl.ds(0, inner - 1), t], w_send, w_recv.at[t], False)

    def biases_arrived():
        if inner > 1:
            await_all(b_buf.at[pl.ds(0, inner - 1)], b_send, b_recv.at[0], False)
        for k in range(1, inner):
            columns(lax.rem(i + k, inner))

    pl.semaphore_wait(barrier, neighbours)
    for load in loads:
        load.wait()
    start_sends(0)
    start_sends(1)
    load_b.wait()
    load_h.wait()
    for k in range(1, inner):
        send_b(k).start()
    load_w.wait()
    for t in range(towers):
        for k in range(1, inner):
            send_w(k, t).start()
    columns(i)
    for h in range(pieces):
        sibling(a, 0, h).start()

    weights = set()
    def far_tasks(s):
        for u, t in far[s]:
            if t not in weights:
                weights.add(t)
                weights_arrived(t)
            group = group_of(u)
            if inner == 2:
                compute(group, lax.rem(i + 1, inner), t, False)
            elif inner > 2:

                def each(k, _, group=group, t=t):
                    compute(group, lax.rem(i + k, inner), t, False)
                    return 0

                lax.fori_loop(1, inner, each, 0)

    for s in range(1, steps):
        for u in own[s]:
            settle(u)
        for u in own[s]:
            for t in range(towers):
                compute(group_of(u), i, t, True)
        take(s - 2)
        start_sends(s + 1)
        if s == 2:
            biases_arrived()
        far_tasks(s)
        ended = []
        for at in range(outer):
            pairs = {}
            for u, (aa, k, q) in enumerate(orders[at]):
                pairs.setdefault((aa, k), []).append(done_at[u])
            ended.append(sorted(p for p, when_done in pairs.items() if max(when_done) == s))
        for n in range(max(len(x) for x in ended)):
            flags = [len(x) > n for x in ended]
            some = next(x[n] for x in ended if len(x) > n)
            entries = [x[n] if len(x) > n else some for x in ended]
            aa = sel([e[0] for e in entries])
            k = sel([e[1] for e in entries])
            when(flags, lambda: give_back(aa, lax.rem(y + k, ys)))

    counts = []
    for at in range(outer):
        each_way = [(ys - 1 if way == 2 or e[1] else 1) for (_, way), e in sends[at].items()]
        counts.append(sum(each_way))
    by_count(counts, lambda n: await_sent(n * piece, x_send))
    await_sent(outer * ys * pieces * piece, core_send)
    if inner > 1:
        await_all(w_buf.at[pl.ds(0, inner - 1)], w_send, w_recv.at[0], True)
        await_all(b_buf.at[pl.ds(0, inner - 1)], b_send, b_recv.at[0], True)
    ret[a * peers + me] = part[a * peers + me]
    await_all(ret.at[pl.ds(0, outer * peers - 1)], p_send, p_recv.at[0], False)
    for pp in range(peers):
        total = ret[pp]
        for aa in range(1, outer):
            total += ret[aa * peers + pp]
        out_ref[pp * towers : (pp + 1) * towers] = total
    await_all(part.at[pl.ds(0, outer * peers - 1)], p_send, p_recv.at[0], True)


def shards(features, task_mask, tower_in, tower_bias, tower_head, head_bias):
    peers, group = lax.axis_size("peer"), lax.axis_size("group")
    rows, depth = features.shape
    towers, hidden, _ = tower_in.shape
    inner = split_of_group(group, peers, tower_in.size, features.size)
    outer = group // inner
    ys = peers // 2
    pieces = rows // PIECE_ROWS
    dma = pltpu.SemaphoreType.DMA
    logits = pl.pallas_call(
        functools.partial(kernel, outer, inner, peers),
        out_shape=pltpu.VMEM((peers * towers, rows), jnp.float32),
        in_specs=[pl.BlockSpec(memory_space=pl.ANY)] * 4
        + [pl.BlockSpec(memory_space=pltpu.SMEM)],
        out_specs=pl.BlockSpec(memory_space=pltpu.VMEM),
        scratch_shapes=[
            pltpu.VMEM((outer * peers * rows, depth), features.dtype),
            pltpu.VMEM((inner, towers, hidden, depth), tower_in.dtype),
            pltpu.VMEM((inner, 2, towers, hidden), tower_bias.dtype),
            pltpu.VMEM((inner, 2, towers, hidden, LANES), jnp.float32),
            pltpu.VMEM((outer * peers, towers, rows), jnp.float32),
            pltpu.VMEM((outer * peers, towers, rows), jnp.float32),
            dma((rows // LANES + 3,)),
            dma((2, plan(outer, pieces)[0])),
            dma((outer * ys * rows // LANES,)),
            dma((1,)),
            dma((1,)),
            dma((1,)),
            dma((towers,)),
            dma((1,)),
            dma((1,)),
            dma((1,)),
            dma((1,)),
        ],
        compiler_params=pltpu.CompilerParams(
            collective_id=0, has_side_effects=True, vmem_limit_bytes=60 * 1024 * 1024
        ),
    )(features, tower_in, tower_bias, tower_head, head_bias)
    tasks = jnp.arange(peers * towers, dtype=jnp.int32)
    bits = (task_mask[:, None] >> tasks[None, :]) & 1
    return jnp.where(bits == 1, logits.T, 0.0)


def solution(mesh):
    placed = (
        P(("group", "peer"), None),
        P(("group", "peer")),
        P("peer", "group", None),
        P("peer", "group"),
        P("peer", "group"),
        P("peer"),
    )
    return jax.shard_map(
        shards, mesh=mesh, in_specs=placed, out_specs=P(("group", "peer"), None), check_vma=False
    )
```

```python
import functools

import jax
import jax.numpy as jnp
from jax import lax
from jax.experimental import pallas as pl
from jax.experimental.pallas import tpu as pltpu
from jax.sharding import PartitionSpec as P

MESH = pl.DeviceIdType.MESH
LANES = 128
PIECE_ROWS = 64
LAG = 3
SLOT_TASKS = 16


def split_of_group(group, peers, weight_bytes, sample_bytes):
    sizes = [f for f in range(1, group + 1) if group % f == 0]

    def cost(f):
        return (f - 1) * weight_bytes + (group // f * peers - 1) * sample_bytes / 2

    return min(sizes, key=cost)


def crosses(outer, pieces, a, aa, h):
    if a == aa:
        return False
    ends = (aa == 0 and a == 1 or aa == outer - 1 and a == outer - 2) and 0 < a < outer - 1
    return ends or h == pieces - 1


def plan(outer, pieces):
    def late(a, aa, h):
        held = a in (0, outer - 1) and h == pieces - 2 and abs(aa - a) in (1, 2)
        return held, -abs(aa - a) if held else 0

    avail = [{(a, 0, h): 0 for h in range(pieces)} for a in range(outer)]
    sends = [{} for _ in range(outer)]
    arrivals = [{} for _ in range(outer)]
    done = set()
    slot = 0
    while any(len(have) < outer * pieces * 2 for have in avail):
        moves = []
        for a in range(outer):
            for way, to in ((0, a + 1), (1, a - 1)):
                if not 0 <= to < outer:
                    continue
                ready = [
                    (k, -abs(aa - to), h, (aa, k, h))
                    for (aa, k, h), since in avail[a].items()
                    if since <= slot
                    and (a, way, aa, k, h) not in done
                    and (aa <= a if way == 0 else aa >= a)
                    and (k == 0 or crosses(outer, pieces, to, aa, h))
                ]
                if ready:
                    moves.append((a, way, to, min(ready)[-1]))
            ready = [
                (*late(a, aa, h), since, h, (aa, 0, h))
                for (aa, k, h), since in avail[a].items()
                if since <= slot
                and k == 0
                and (a, 2, aa, k, h) not in done
                and not crosses(outer, pieces, a, aa, h)
            ]
            if ready:
                moves.append((a, 2, a, min(ready)[-1]))
        for a, way, to, (aa, k, h) in moves:
            done.add((a, way, aa, k, h))
            sends[a].setdefault((slot, way), (aa, k, h))
            got = (aa, 1 if way == 2 else k, h)
            avail[to][got] = slot + LAG
            arrivals[to].setdefault(slot, []).append(got)
        slot += 1
    return slot, sends, arrivals, avail


def tasks_of(outer, ys, pieces, towers, ready_far, avail):
    per = LANES // PIECE_ROWS
    orders = []
    for a in range(outer):
        groups = []
        for aa in range(outer):
            for k in range(ys):
                for q in range(pieces // per):
                    at = max(avail[a][aa, min(k, 1), h] for h in range(q * per, (q + 1) * per))
                    groups.append((max(at, 1), abs(aa - a), k, q, aa))
        orders.append(sorted(groups))
    count = len(orders[0])
    at = [max(orders[a][u][0] for a in range(outer)) for u in range(count)]
    at = [max(at[: u + 1]) for u in range(count)]
    last = at[-1]
    own = [[u for u in range(count) if at[u] == s] for s in range(last + 1)]
    far = []
    left = [(u, t) for t in range(towers) for u in range(count)]
    for s in range(last + 1):
        room = 10**6 if s == last else SLOT_TASKS - towers * len(own[s])
        now = [(u, t) for (u, t) in left if at[u] <= s and min(ready_far[t], last) <= s][: max(room, 0)]
        far.append(now)
        left = [x for x in left if x not in now]
    assert not left
    return [[(aa, k, q) for _, _, k, q, aa in order] for order in orders], own, far


def kernel(
    outer, inner, peers,
    feat_ref, weight_ref, bias_ref, head_ref, hbias_ref, out_ref,
    x_buf, w_buf, b_buf, c_buf, h_buf, part, ret,
    load_sem, x_recv, core_recv, x_send, core_send, w_send, w_recv, b_send, b_recv, p_send, p_recv,
):
    rows, depth = feat_ref.shape
    towers, hidden, _ = weight_ref.shape
    piece = PIECE_ROWS
    pieces = rows // piece
    per = LANES // piece
    quads = rows // LANES
    ys = peers // 2
    group_at, me = lax.axis_index("group"), lax.axis_index("peer")
    a, i = group_at // inner, group_at % inner
    y, c = me // 2, me % 2
    partner = y * 2 + (1 - c)

    def dev(a_to, i_to, p_to):
        return (a_to * inner + i_to, p_to)

    def sel(values):
        out = values[-1]
        for at in range(outer - 2, -1, -1):
            if not isinstance(out, int) or values[at] != out:
                out = jnp.where(a == at, values[at], out)
        return out

    def when(flags, do):
        if all(flags):
            do()
        elif any(flags):
            pl.when(sel([int(f) for f in flags]) == 1)(do)

    def at_group(aa, yy, q):
        return (aa * ys + yy) * quads + q

    def x_rows(aa, yy, q, cc, start=0, size=LANES):
        row = (at_group(aa, yy, q) * 2 + cc) * LANES + start
        return x_buf.at[pl.ds(pl.multiple_of(row, PIECE_ROWS), size)]

    loads = [
        pltpu.make_async_copy(
            feat_ref.at[pl.ds(q * LANES, LANES)], x_rows(a, y, q, c), load_sem.at[0]
        )
        for q in range(quads)
    ]
    load_w = pltpu.make_async_copy(weight_ref, w_buf.at[i], load_sem.at[1])
    load_b = pltpu.make_async_copy(bias_ref, b_buf.at[i, 0], load_sem.at[2])
    load_h = pltpu.make_async_copy(head_ref, b_buf.at[i, 1], load_sem.at[2])
    load_s = pltpu.make_async_copy(hbias_ref, h_buf, load_sem.at[3])
    barrier = pltpu.get_barrier_semaphore()

    def greet(to):
        pl.semaphore_signal(barrier, inc=1, device_id=to, device_id_type=MESH)

    pl.when(a + 1 < outer)(lambda: greet(dev(lax.rem(a + 1, outer), i, me)))
    pl.when(a > 0)(lambda: greet(dev(lax.rem(a + outer - 1, outer), i, me)))
    for k in range(1, ys):
        greet(dev(a, i, lax.rem(y + k, ys) * 2 + c))
    for k in range(1, inner):
        greet(dev(a, lax.rem(i + k, inner), me))
    greet(dev(a, i, partner))
    for load in loads:
        load.start()
    load_w.start()
    load_b.start()
    load_h.start()
    load_s.start()
    neighbours = sel([(at > 0) + (at + 1 < outer) + ys + inner - 1 for at in range(outer)])

    def column(k):
        return lax.rem(y + k, ys) if k else y

    def send_x(aa, yy, h, send_sem, recv_sem, to):
        ref = x_rows(aa, yy, h // per, c, h % per * piece, piece)
        return pltpu.make_async_remote_copy(
            src_ref=ref, dst_ref=ref, send_sem=send_sem, recv_sem=recv_sem,
            device_id=to, device_id_type=MESH,
        )

    def along(way, aa, k, h, slot):
        to = lax.rem(a + 1, outer) if way == 0 else lax.rem(a + outer - 1, outer)
        return send_x(aa, column(k), h, x_send.at[0], x_recv.at[slot], dev(to, i, me))

    def across(aa, k, h, slot):
        to = dev(a, i, lax.rem(y + k, ys) * 2 + c)
        return send_x(aa, y, h, x_send.at[0], x_recv.at[slot], to)

    def sibling(aa, k, h):
        sem = core_recv.at[at_group(aa, column(k), h // per)]
        return send_x(aa, column(k), h, core_send.at[0], sem, dev(a, i, partner))

    def await_rows(count, sem):
        ref = x_buf.at[pl.ds(0, count)]
        pltpu.make_async_remote_copy(
            src_ref=ref, dst_ref=ref, send_sem=x_send.at[0], recv_sem=sem,
            device_id=dev(a, i, partner), device_id_type=MESH,
        ).wait_recv()

    def await_sent(count, sem):
        ref = x_buf.at[pl.ds(0, count)]
        pltpu.make_async_remote_copy(
            src_ref=ref, dst_ref=ref, send_sem=sem.at[0], recv_sem=p_recv.at[0],
            device_id=dev(a, i, partner), device_id_type=MESH,
        ).wait_send()

    def send_w(k, t):
        return pltpu.make_async_remote_copy(
            src_ref=w_buf.at[i, t], dst_ref=w_buf.at[i, t], send_sem=w_send.at[0],
            recv_sem=w_recv.at[t], device_id=dev(a, lax.rem(i + k, inner), me), device_id_type=MESH,
        )

    def send_b(k):
        return pltpu.make_async_remote_copy(
            src_ref=b_buf.at[i], dst_ref=b_buf.at[i], send_sem=b_send.at[0],
            recv_sem=b_recv.at[0], device_id=dev(a, lax.rem(i + k, inner), me), device_id_type=MESH,
        )

    def await_all(ref, send_sem, recv_sem, sent):
        copy = pltpu.make_async_remote_copy(
            src_ref=ref, dst_ref=ref, send_sem=send_sem.at[0], recv_sem=recv_sem,
            device_id=dev(a, i, partner), device_id_type=MESH,
        )
        copy.wait_send() if sent else copy.wait_recv()

    def columns(ii):
        diagonal = lax.broadcasted_iota(jnp.int32, (hidden, hidden), 0) == (
            lax.broadcasted_iota(jnp.int32, (hidden, hidden), 1)
        )
        for w in range(2):
            both = b_buf[ii, w].astype(jnp.float32)
            for t in range(towers):
                picked = jnp.where(diagonal, both[t : t + 1], 0.0)
                total = jnp.sum(picked, axis=1, keepdims=True)
                c_buf[ii, w, t] = jnp.broadcast_to(total, (hidden, LANES))

    def compute(group, ii, t, first):
        aa, yy, q = group
        row = pl.multiple_of(at_group(aa, yy, q) * 2 * LANES, 2 * LANES)
        x = x_buf[pl.ds(row, 2 * LANES)]
        pre = lax.dot_general(
            w_buf[ii, t], x, (((1,), (1,)), ((), ())), preferred_element_type=jnp.float32
        )
        bias, head = c_buf[ii, 0, t], c_buf[ii, 1, t]
        lanes = pl.ds(pl.multiple_of(q * LANES, LANES), LANES)
        for cc in range(2):
            v = jnp.maximum(pre[:, cc * LANES : (cc + 1) * LANES] + bias, 0.0) * head
            total = jnp.sum(v, axis=0, keepdims=True)
            if first:
                total += jnp.where(a == 0, h_buf[t], 0.0)
            else:
                total += part[aa * peers + yy * 2 + cc, pl.ds(t, 1), lanes]
            part[aa * peers + yy * 2 + cc, pl.ds(t, 1), lanes] = total

    def send_part(aa, pp):
        return pltpu.make_async_remote_copy(
            src_ref=part.at[aa * peers + pp], dst_ref=ret.at[a * peers + me],
            send_sem=p_send.at[0], recv_sem=p_recv.at[0],
            device_id=dev(aa, i, pp), device_id_type=MESH,
        )

    def give_back(aa, yy):
        for cc in range(2):
            pp = yy * 2 + cc
            mine = (aa == a) & (pp == me)
            pl.when(jnp.logical_not(mine))(lambda pp=pp: send_part(aa, pp).start())

    slots, sends, arrivals, avail = plan(outer, pieces)
    ready_far = [-(-hidden * max(inner - 1, 1) * (t + 1) // piece) + 1 for t in range(towers)]
    orders, own, far = tasks_of(outer, ys, pieces, towers, ready_far, avail)
    steps = len(own)
    done_at = {}
    for s in range(steps):
        for u in own[s]:
            done_at[u] = s
        for u, _ in far[s]:
            done_at[u] = s

    def group_of(u):
        aa = sel([orders[at][u][0] for at in range(outer)])
        k = sel([orders[at][u][1] for at in range(outer)])
        q = sel([orders[at][u][2] for at in range(outer)])
        return aa, (lax.rem(y + k, ys) if not isinstance(k, int) or k else y), q

    def start_sends(slot):
        for way in range(3):
            entries = [sends[at].get((slot, way)) for at in range(outer)]
            flags = [e is not None for e in entries]
            if not any(flags):
                continue
            some = next(e for e in entries if e is not None)
            entries = [e or some for e in entries]
            issue_sends(way, entries, flags, slot)

    def issue_sends(way, entries, flags, slot):
        aa = sel([e[0] for e in entries])
        h = sel([e[2] for e in entries])
        kinds = sorted({e[1] for e, f in zip(entries, flags) if f})

        for kind in kinds:

            def go(kind=kind):
                for k in range(1, ys) if way == 2 or kind else (0,):
                    copy = across(aa, k, h, slot) if way == 2 else along(way, aa, k, h, slot)
                    copy.start()

            when([f and e[1] == kind for e, f in zip(entries, flags)], go)

    def by_count(counts, do):
        for count in sorted(set(counts) - {0}):
            when([n == count for n in counts], lambda count=count: do(count))

    def take(slot):
        lists = [arrivals[at].get(slot, []) for at in range(outer)]
        counts = [sum(ys - 1 if k else 1 for _, k, _ in x) for x in lists]
        by_count(counts, lambda n: await_rows(n * piece, x_recv.at[slot]))
        for n in range(max(len(x) for x in lists)):
            for kind in range(2):
                flags = [len(x) > n and x[n][1] == kind for x in lists]
                if not any(flags):
                    continue
                some = next(x[n] for x, f in zip(lists, flags) if f)
                entries = [x[n] if f else some for x, f in zip(lists, flags)]
                aa = sel([e[0] for e in entries])
                h = sel([e[2] for e in entries])

                def relay(aa=aa, h=h, kind=kind):
                    for k in range(1, ys) if kind else (0,):
                        sibling(aa, k, h).start()

                when(flags, relay)

    def settle(u):
        await_rows(LANES, core_recv.at[at_group(*group_of(u))])

    def weights_arrived(t):
        if inner > 1:
            await_all(w_buf.at[pl.ds(0, inner - 1), t], w_send, w_recv.at[t], False)

    def biases_arrived():
        if inner > 1:
            await_all(b_buf.at[pl.ds(0, inner - 1)], b_send, b_recv.at[0], False)
        for k in range(1, inner):
            columns(lax.rem(i + k, inner))

    pl.semaphore_wait(barrier, neighbours)
    pltpu.make_async_copy(feat_ref, x_buf.at[pl.ds(0, rows)], load_sem.at[0]).wait()
    start_sends(0)
    start_sends(1)
    pltpu.make_async_copy(b_buf.at[i], b_buf.at[i], load_sem.at[2]).wait()
    load_s.wait()
    for k in range(1, inner):
        send_b(k).start()
    load_w.wait()
    for t in range(towers):
        for k in range(1, inner):
            send_w(k, t).start()
    columns(i)
    for h in range(pieces):
        sibling(a, 0, h).start()

    weights = set()
    def far_tasks(s):
        for u, t in far[s]:
            if t not in weights:
                weights.add(t)
                weights_arrived(t)
            group = group_of(u)
            if inner == 2:
                compute(group, lax.rem(i + 1, inner), t, False)
            elif inner > 2:

                def each(k, _, group=group, t=t):
                    compute(group, lax.rem(i + k, inner), t, False)
                    return 0

                lax.fori_loop(1, inner, each, 0)

    for s in range(1, steps):
        for u in own[s]:
            settle(u)
        for u in own[s]:
            for t in range(towers):
                compute(group_of(u), i, t, True)
        take(s - 2)
        start_sends(s + 1)
        if s == 2:
            biases_arrived()
        far_tasks(s)
        ended = []
        for at in range(outer):
            pairs = {}
            for u, (aa, k, q) in enumerate(orders[at]):
                pairs.setdefault((aa, k), []).append(done_at[u])
            ended.append(sorted(p for p, when_done in pairs.items() if max(when_done) == s))
        for n in range(max(len(x) for x in ended)):
            flags = [len(x) > n for x in ended]
            some = next(x[n] for x in ended if len(x) > n)
            entries = [x[n] if len(x) > n else some for x in ended]
            aa = sel([e[0] for e in entries])
            k = sel([e[1] for e in entries])
            when(flags, lambda: give_back(aa, lax.rem(y + k, ys)))

    counts = []
    for at in range(outer):
        each_way = [(ys - 1 if way == 2 or e[1] else 1) for (_, way), e in sends[at].items()]
        counts.append(sum(each_way))
    by_count(counts, lambda n: await_sent(n * piece, x_send))
    await_sent(outer * ys * pieces * piece, core_send)
    if inner > 1:
        await_all(w_buf.at[pl.ds(0, inner - 1)], w_send, w_recv.at[0], True)
        await_all(b_buf.at[pl.ds(0, inner - 1)], b_send, b_recv.at[0], True)
    ret[a * peers + me] = part[a * peers + me]
    await_all(ret.at[pl.ds(0, outer * peers - 1)], p_send, p_recv.at[0], False)
    for pp in range(peers):
        total = ret[pp]
        for aa in range(1, outer):
            total += ret[aa * peers + pp]
        out_ref[pp * towers : (pp + 1) * towers] = total
    await_all(part.at[pl.ds(0, outer * peers - 1)], p_send, p_recv.at[0], True)


def shards(features, task_mask, tower_in, tower_bias, tower_head, head_bias):
    peers, group = lax.axis_size("peer"), lax.axis_size("group")
    rows, depth = features.shape
    towers, hidden, _ = tower_in.shape
    inner = split_of_group(group, peers, tower_in.size, features.size)
    outer = group // inner
    ys = peers // 2
    pieces = rows // PIECE_ROWS
    dma = pltpu.SemaphoreType.DMA
    logits = pl.pallas_call(
        functools.partial(kernel, outer, inner, peers),
        out_shape=pltpu.VMEM((peers * towers, rows), jnp.float32),
        in_specs=[pl.BlockSpec(memory_space=pl.ANY)] * 5,
        out_specs=pl.BlockSpec(memory_space=pltpu.VMEM),
        scratch_shapes=[
            pltpu.VMEM((outer * peers * rows, depth), features.dtype),
            pltpu.VMEM((inner, towers, hidden, depth), tower_in.dtype),
            pltpu.VMEM((inner, 2, towers, hidden), tower_bias.dtype),
            pltpu.VMEM((inner, 2, towers, hidden, LANES), jnp.float32),
            pltpu.SMEM((towers,), jnp.float32),
            pltpu.VMEM((outer * peers, towers, rows), jnp.float32),
            pltpu.VMEM((outer * peers, towers, rows), jnp.float32),
            dma((4,)),
            dma((plan(outer, pieces)[0],)),
            dma((outer * ys * rows // LANES,)),
            dma((1,)),
            dma((1,)),
            dma((1,)),
            dma((towers,)),
            dma((1,)),
            dma((1,)),
            dma((1,)),
            dma((1,)),
        ],
        compiler_params=pltpu.CompilerParams(
            collective_id=0, has_side_effects=True, vmem_limit_bytes=60 * 1024 * 1024
        ),
    )(features, tower_in, tower_bias, tower_head, head_bias)
    tasks = jnp.arange(peers * towers, dtype=jnp.int32)
    bits = (task_mask[:, None] >> tasks[None, :]) & 1
    return jnp.where(bits == 1, logits.T, 0.0)


def solution(mesh):
    placed = (
        P(("group", "peer"), None),
        P(("group", "peer")),
        P("peer", "group", None),
        P("peer", "group"),
        P("peer", "group"),
        P("peer"),
    )
    return jax.shard_map(
        shards, mesh=mesh, in_specs=placed, out_specs=P(("group", "peer"), None), check_vma=False
    )
```

```python
import functools

import jax
import jax.numpy as jnp
from jax import lax
from jax.experimental import pallas as pl
from jax.experimental.pallas import tpu as pltpu
from jax.sharding import PartitionSpec as P

MESH = pl.DeviceIdType.MESH
LANES = 128
PIECE_ROWS = 64
LAG = 3
SLOT_TASKS = 16


def split_of_group(group, peers, weight_bytes, sample_bytes):
    sizes = [f for f in range(1, group + 1) if group % f == 0]

    def cost(f):
        return (f - 1) * weight_bytes + (group // f * peers - 1) * sample_bytes / 2

    return min(sizes, key=cost)


def crosses(outer, pieces, a, aa, h):
    if a == aa:
        return False
    ends = (aa == 0 and a == 1 or aa == outer - 1 and a == outer - 2) and 0 < a < outer - 1
    return ends or h == pieces - 1


def plan(outer, pieces):
    def late(a, aa, h):
        held = a in (0, outer - 1) and h == pieces - 2 and abs(aa - a) in (1, 2)
        return held, -abs(aa - a) if held else 0

    avail = [{(a, 0, h): 0 for h in range(pieces)} for a in range(outer)]
    sends = [{} for _ in range(outer)]
    arrivals = [{} for _ in range(outer)]
    done = set()
    slot = 0
    while any(len(have) < outer * pieces * 2 for have in avail):
        moves = []
        for a in range(outer):
            for way, to in ((0, a + 1), (1, a - 1)):
                if not 0 <= to < outer:
                    continue
                ready = [
                    (k, -abs(aa - to), h, (aa, k, h))
                    for (aa, k, h), since in avail[a].items()
                    if since <= slot
                    and (a, way, aa, k, h) not in done
                    and (aa <= a if way == 0 else aa >= a)
                    and (k == 0 or crosses(outer, pieces, to, aa, h))
                ]
                if ready:
                    moves.append((a, way, to, min(ready)[-1]))
            ready = [
                (*late(a, aa, h), since, h, (aa, 0, h))
                for (aa, k, h), since in avail[a].items()
                if since <= slot
                and k == 0
                and (a, 2, aa, k, h) not in done
                and not crosses(outer, pieces, a, aa, h)
            ]
            if ready:
                moves.append((a, 2, a, min(ready)[-1]))
        for a, way, to, (aa, k, h) in moves:
            done.add((a, way, aa, k, h))
            sends[a].setdefault((slot, way), (aa, k, h))
            got = (aa, 1 if way == 2 else k, h)
            avail[to][got] = slot + LAG
            arrivals[to].setdefault(slot, []).append(got)
        slot += 1
    return slot, sends, arrivals, avail


def tasks_of(outer, ys, pieces, towers, ready_far, avail):
    per = LANES // PIECE_ROWS
    orders = []
    for a in range(outer):
        groups = []
        for aa in range(outer):
            for k in range(ys):
                for q in range(pieces // per):
                    at = max(avail[a][aa, min(k, 1), h] for h in range(q * per, (q + 1) * per))
                    groups.append((max(at, 1), abs(aa - a), k, q, aa))
        orders.append(sorted(groups))
    count = len(orders[0])
    at = [max(orders[a][u][0] for a in range(outer)) for u in range(count)]
    at = [max(at[: u + 1]) for u in range(count)]
    last = at[-1]
    own = [[u for u in range(count) if at[u] == s] for s in range(last + 1)]
    far = []
    left = [(u, t) for t in range(towers) for u in range(count)]
    for s in range(last + 1):
        room = 10**6 if s == last else SLOT_TASKS - towers * len(own[s])
        now = [(u, t) for (u, t) in left if at[u] <= s and min(ready_far[t], last) <= s][: max(room, 0)]
        far.append(now)
        left = [x for x in left if x not in now]
    assert not left
    return [[(aa, k, q) for _, _, k, q, aa in order] for order in orders], own, far


def kernel(
    outer, inner, peers,
    feat_ref, weight_ref, bias_ref, head_ref, hbias_ref, out_ref,
    x_buf, w_buf, b_buf, c_buf, h_buf, part, ret,
    load_sem, x_recv, core_recv, x_send, core_send, w_send, w_recv, b_send, b_recv, p_send, p_recv,
):
    rows, depth = feat_ref.shape
    towers, hidden, _ = weight_ref.shape
    piece = PIECE_ROWS
    pieces = rows // piece
    per = LANES // piece
    quads = rows // LANES
    ys = peers // 2
    group_at, me = lax.axis_index("group"), lax.axis_index("peer")
    a, i = group_at // inner, group_at % inner
    y, c = me // 2, me % 2
    partner = y * 2 + (1 - c)

    def dev(a_to, i_to, p_to):
        return (a_to * inner + i_to, p_to)

    def sel(values):
        out = values[-1]
        for at in range(outer - 2, -1, -1):
            if not isinstance(out, int) or values[at] != out:
                out = jnp.where(a == at, values[at], out)
        return out

    def when(flags, do):
        if all(flags):
            do()
        elif any(flags):
            pl.when(sel([int(f) for f in flags]) == 1)(do)

    def at_group(aa, yy, q):
        return (aa * ys + yy) * quads + q

    def x_rows(aa, yy, q, cc, start=0, size=LANES):
        row = (at_group(aa, yy, q) * 2 + cc) * LANES + start
        return x_buf.at[pl.ds(pl.multiple_of(row, PIECE_ROWS), size)]

    loads = [
        pltpu.make_async_copy(
            feat_ref.at[pl.ds(q * LANES, LANES)], x_rows(a, y, q, c), load_sem.at[0]
        )
        for q in range(quads)
    ]
    load_w = pltpu.make_async_copy(weight_ref, w_buf.at[i], load_sem.at[1])
    load_b = pltpu.make_async_copy(bias_ref, b_buf.at[i, 0], load_sem.at[2])
    load_h = pltpu.make_async_copy(head_ref, b_buf.at[i, 1], load_sem.at[2])
    load_s = pltpu.make_async_copy(hbias_ref, h_buf, load_sem.at[3])
    barrier = pltpu.get_barrier_semaphore()

    def greet(to):
        pl.semaphore_signal(barrier, inc=1, device_id=to, device_id_type=MESH)

    pl.when(a + 1 < outer)(lambda: greet(dev(lax.rem(a + 1, outer), i, me)))
    pl.when(a > 0)(lambda: greet(dev(lax.rem(a + outer - 1, outer), i, me)))
    for k in range(1, ys):
        greet(dev(a, i, lax.rem(y + k, ys) * 2 + c))
    for k in range(1, inner):
        greet(dev(a, lax.rem(i + k, inner), me))
    greet(dev(a, i, partner))
    for load in loads:
        load.start()
    load_w.start()
    load_b.start()
    load_h.start()
    load_s.start()
    neighbours = sel([(at > 0) + (at + 1 < outer) + ys + inner - 1 for at in range(outer)])

    def column(k):
        return lax.rem(y + k, ys) if k else y

    def send_x(aa, yy, h, send_sem, recv_sem, to):
        ref = x_rows(aa, yy, h // per, c, h % per * piece, piece)
        return pltpu.make_async_remote_copy(
            src_ref=ref, dst_ref=ref, send_sem=send_sem, recv_sem=recv_sem,
            device_id=to, device_id_type=MESH,
        )

    def along(way, aa, k, h, slot):
        to = lax.rem(a + 1, outer) if way == 0 else lax.rem(a + outer - 1, outer)
        return send_x(aa, column(k), h, x_send.at[0], x_recv.at[slot], dev(to, i, me))

    def across(aa, k, h, slot):
        to = dev(a, i, lax.rem(y + k, ys) * 2 + c)
        return send_x(aa, y, h, x_send.at[0], x_recv.at[slot], to)

    def sibling(aa, k, h, used):
        return send_x(aa, column(k), h, core_send.at[0], core_recv.at[used], dev(a, i, partner))

    def await_rows(count, sem):
        ref = x_buf.at[pl.ds(0, count)]
        pltpu.make_async_remote_copy(
            src_ref=ref, dst_ref=ref, send_sem=x_send.at[0], recv_sem=sem,
            device_id=dev(a, i, partner), device_id_type=MESH,
        ).wait_recv()

    def await_sent(count, sem):
        ref = x_buf.at[pl.ds(0, count)]
        pltpu.make_async_remote_copy(
            src_ref=ref, dst_ref=ref, send_sem=sem.at[0], recv_sem=p_recv.at[0],
            device_id=dev(a, i, partner), device_id_type=MESH,
        ).wait_send()

    def send_w(k, t):
        return pltpu.make_async_remote_copy(
            src_ref=w_buf.at[i, t], dst_ref=w_buf.at[i, t], send_sem=w_send.at[0],
            recv_sem=w_recv.at[t], device_id=dev(a, lax.rem(i + k, inner), me), device_id_type=MESH,
        )

    def send_b(k):
        return pltpu.make_async_remote_copy(
            src_ref=b_buf.at[i], dst_ref=b_buf.at[i], send_sem=b_send.at[0],
            recv_sem=b_recv.at[0], device_id=dev(a, lax.rem(i + k, inner), me), device_id_type=MESH,
        )

    def await_all(ref, send_sem, recv_sem, sent):
        copy = pltpu.make_async_remote_copy(
            src_ref=ref, dst_ref=ref, send_sem=send_sem.at[0], recv_sem=recv_sem,
            device_id=dev(a, i, partner), device_id_type=MESH,
        )
        copy.wait_send() if sent else copy.wait_recv()

    def columns(ii):
        diagonal = lax.broadcasted_iota(jnp.int32, (hidden, hidden), 0) == (
            lax.broadcasted_iota(jnp.int32, (hidden, hidden), 1)
        )
        for w in range(2):
            both = b_buf[ii, w].astype(jnp.float32)
            for t in range(towers):
                picked = jnp.where(diagonal, both[t : t + 1], 0.0)
                total = jnp.sum(picked, axis=1, keepdims=True)
                c_buf[ii, w, t] = jnp.broadcast_to(total, (hidden, LANES))

    def compute(group, ii, t, first):
        aa, yy, q = group
        row = pl.multiple_of(at_group(aa, yy, q) * 2 * LANES, 2 * LANES)
        x = x_buf[pl.ds(row, 2 * LANES)]
        pre = lax.dot_general(
            w_buf[ii, t], x, (((1,), (1,)), ((), ())), preferred_element_type=jnp.float32
        )
        bias, head = c_buf[ii, 0, t], c_buf[ii, 1, t]
        lanes = pl.ds(pl.multiple_of(q * LANES, LANES), LANES)
        for cc in range(2):
            v = jnp.maximum(pre[:, cc * LANES : (cc + 1) * LANES] + bias, 0.0) * head
            total = jnp.sum(v, axis=0, keepdims=True)
            if first:
                total += jnp.where(a == 0, h_buf[t], 0.0)
            else:
                total += part[aa * peers + yy * 2 + cc, pl.ds(t, 1), lanes]
            part[aa * peers + yy * 2 + cc, pl.ds(t, 1), lanes] = total

    def send_part(aa, pp):
        return pltpu.make_async_remote_copy(
            src_ref=part.at[aa * peers + pp], dst_ref=ret.at[a * peers + me],
            send_sem=p_send.at[0], recv_sem=p_recv.at[0],
            device_id=dev(aa, i, pp), device_id_type=MESH,
        )

    def give_back(aa, yy):
        for cc in range(2):
            pp = yy * 2 + cc
            mine = (aa == a) & (pp == me)
            pl.when(jnp.logical_not(mine))(lambda pp=pp: send_part(aa, pp).start())

    slots, sends, arrivals, avail = plan(outer, pieces)
    ready_far = [-(-hidden * max(inner - 1, 1) * (t + 1) // piece) + 1 for t in range(towers)]
    orders, own, far = tasks_of(outer, ys, pieces, towers, ready_far, avail)
    steps = len(own)
    done_at = {}
    for s in range(steps):
        for u in own[s]:
            done_at[u] = s
        for u, _ in far[s]:
            done_at[u] = s

    used_steps = [s for s in range(steps) if own[s]]
    used_at = [
        {order[u]: n for n, s in enumerate(used_steps) for u in own[s]} for order in orders
    ]

    def used_by(entries, k):
        return sel([used_at[at][e[0], k, e[2] // per] for at, e in enumerate(entries)])

    def group_of(u):
        aa = sel([orders[at][u][0] for at in range(outer)])
        k = sel([orders[at][u][1] for at in range(outer)])
        q = sel([orders[at][u][2] for at in range(outer)])
        return aa, (lax.rem(y + k, ys) if not isinstance(k, int) or k else y), q

    def start_sends(slot):
        for way in range(3):
            entries = [sends[at].get((slot, way)) for at in range(outer)]
            flags = [e is not None for e in entries]
            if not any(flags):
                continue
            some = next(e for e in entries if e is not None)
            entries = [e or some for e in entries]
            issue_sends(way, entries, flags, slot)

    def issue_sends(way, entries, flags, slot):
        aa = sel([e[0] for e in entries])
        h = sel([e[2] for e in entries])
        kinds = sorted({e[1] for e, f in zip(entries, flags) if f})

        for kind in kinds:

            def go(kind=kind):
                for k in range(1, ys) if way == 2 or kind else (0,):
                    copy = across(aa, k, h, slot) if way == 2 else along(way, aa, k, h, slot)
                    copy.start()

            when([f and e[1] == kind for e, f in zip(entries, flags)], go)

    def by_count(counts, do):
        for count in sorted(set(counts) - {0}):
            when([n == count for n in counts], lambda count=count: do(count))

    def take(slot):
        lists = [arrivals[at].get(slot, []) for at in range(outer)]
        counts = [sum(ys - 1 if k else 1 for _, k, _ in x) for x in lists]
        by_count(counts, lambda n: await_rows(n * piece, x_recv.at[slot]))
        for n in range(max(len(x) for x in lists)):
            for kind in range(2):
                flags = [len(x) > n and x[n][1] == kind for x in lists]
                if not any(flags):
                    continue
                some = next(x[n] for x, f in zip(lists, flags) if f)
                entries = [x[n] if f else some for x, f in zip(lists, flags)]
                aa = sel([e[0] for e in entries])
                h = sel([e[2] for e in entries])

                def relay(aa=aa, h=h, kind=kind, entries=entries):
                    for k in range(1, ys) if kind else (0,):
                        sibling(aa, k, h, used_by(entries, k)).start()

                when(flags, relay)

    def settle(s):
        await_rows(len(own[s]) * LANES, core_recv.at[used_steps.index(s)])

    def weights_arrived(t):
        if inner > 1:
            await_all(w_buf.at[pl.ds(0, inner - 1), t], w_send, w_recv.at[t], False)

    def biases_arrived():
        if inner > 1:
            await_all(b_buf.at[pl.ds(0, inner - 1)], b_send, b_recv.at[0], False)
        for k in range(1, inner):
            columns(lax.rem(i + k, inner))

    pl.semaphore_wait(barrier, neighbours)
    pltpu.make_async_copy(feat_ref, x_buf.at[pl.ds(0, rows)], load_sem.at[0]).wait()
    start_sends(0)
    start_sends(1)
    pltpu.make_async_copy(b_buf.at[i], b_buf.at[i], load_sem.at[2]).wait()
    load_s.wait()
    for k in range(1, inner):
        send_b(k).start()
    load_w.wait()
    for t in range(towers):
        for k in range(1, inner):
            send_w(k, t).start()
    columns(i)
    for h in range(pieces):
        sibling(a, 0, h, used_by([(at, 0, h) for at in range(outer)], 0)).start()

    weights = set()
    def far_tasks(s):
        for u, t in far[s]:
            if t not in weights:
                weights.add(t)
                weights_arrived(t)
            group = group_of(u)
            if inner == 2:
                compute(group, lax.rem(i + 1, inner), t, False)
            elif inner > 2:

                def each(k, _, group=group, t=t):
                    compute(group, lax.rem(i + k, inner), t, False)
                    return 0

                lax.fori_loop(1, inner, each, 0)

    for s in range(1, steps):
        if own[s]:
            settle(s)
        for u in own[s]:
            for t in range(towers):
                compute(group_of(u), i, t, True)
        take(s - 2)
        start_sends(s + 1)
        if s == 2:
            biases_arrived()
        far_tasks(s)
        ended = []
        for at in range(outer):
            pairs = {}
            for u, (aa, k, q) in enumerate(orders[at]):
                pairs.setdefault((aa, k), []).append(done_at[u])
            ended.append(sorted(p for p, when_done in pairs.items() if max(when_done) == s))
        for n in range(max(len(x) for x in ended)):
            flags = [len(x) > n for x in ended]
            some = next(x[n] for x in ended if len(x) > n)
            entries = [x[n] if len(x) > n else some for x in ended]
            aa = sel([e[0] for e in entries])
            k = sel([e[1] for e in entries])
            when(flags, lambda: give_back(aa, lax.rem(y + k, ys)))

    counts = []
    for at in range(outer):
        each_way = [(ys - 1 if way == 2 or e[1] else 1) for (_, way), e in sends[at].items()]
        counts.append(sum(each_way))
    by_count(counts, lambda n: await_sent(n * piece, x_send))
    await_sent(outer * ys * pieces * piece, core_send)
    if inner > 1:
        await_all(w_buf.at[pl.ds(0, inner - 1)], w_send, w_recv.at[0], True)
        await_all(b_buf.at[pl.ds(0, inner - 1)], b_send, b_recv.at[0], True)
    ret[a * peers + me] = part[a * peers + me]
    await_all(ret.at[pl.ds(0, outer * peers - 1)], p_send, p_recv.at[0], False)
    for pp in range(peers):
        total = ret[pp]
        for aa in range(1, outer):
            total += ret[aa * peers + pp]
        out_ref[pp * towers : (pp + 1) * towers] = total
    await_all(part.at[pl.ds(0, outer * peers - 1)], p_send, p_recv.at[0], True)


def shards(features, task_mask, tower_in, tower_bias, tower_head, head_bias):
    peers, group = lax.axis_size("peer"), lax.axis_size("group")
    rows, depth = features.shape
    towers, hidden, _ = tower_in.shape
    inner = split_of_group(group, peers, tower_in.size, features.size)
    outer = group // inner
    ys = peers // 2
    pieces = rows // PIECE_ROWS
    slots, _, _, avail = plan(outer, pieces)
    own = tasks_of(outer, ys, pieces, towers, [0] * towers, avail)[1]
    used = sum(1 for groups in own if groups)
    dma = pltpu.SemaphoreType.DMA
    logits = pl.pallas_call(
        functools.partial(kernel, outer, inner, peers),
        out_shape=pltpu.VMEM((peers * towers, rows), jnp.float32),
        in_specs=[pl.BlockSpec(memory_space=pl.ANY)] * 5,
        out_specs=pl.BlockSpec(memory_space=pltpu.VMEM),
        scratch_shapes=[
            pltpu.VMEM((outer * peers * rows, depth), features.dtype),
            pltpu.VMEM((inner, towers, hidden, depth), tower_in.dtype),
            pltpu.VMEM((inner, 2, towers, hidden), tower_bias.dtype),
            pltpu.VMEM((inner, 2, towers, hidden, LANES), jnp.float32),
            pltpu.SMEM((towers,), jnp.float32),
            pltpu.VMEM((outer * peers, towers, rows), jnp.float32),
            pltpu.VMEM((outer * peers, towers, rows), jnp.float32),
            dma((4,)),
            dma((slots,)),
            dma((used,)),
            dma((1,)),
            dma((1,)),
            dma((1,)),
            dma((towers,)),
            dma((1,)),
            dma((1,)),
            dma((1,)),
            dma((1,)),
        ],
        compiler_params=pltpu.CompilerParams(
            collective_id=0, has_side_effects=True, vmem_limit_bytes=60 * 1024 * 1024
        ),
    )(features, tower_in, tower_bias, tower_head, head_bias)
    tasks = jnp.arange(peers * towers, dtype=jnp.int32)
    bits = (task_mask[:, None] >> tasks[None, :]) & 1
    return jnp.where(bits == 1, logits.T, 0.0)


def solution(mesh):
    placed = (
        P(("group", "peer"), None),
        P(("group", "peer")),
        P("peer", "group", None),
        P("peer", "group"),
        P("peer", "group"),
        P("peer"),
    )
    return jax.shard_map(
        shards, mesh=mesh, in_specs=placed, out_specs=P(("group", "peer"), None), check_vma=False
    )
```
